256 devices in a mesh: dp: 2 (over y_hi), tm: 32 (over z, y_lo, core), rows: 4 (over x).
Axes of the slice: x: 4, y: 4 (y_hi: 2, y_lo: 2; y = y_hi * 2 + y_lo), z: 8, core: 2. Of those that a mesh axis runs over, the one named last changes fastest.
Arguments:
- clips: bfloat16 [2, 64, 4, 128, 256], P('dp', 'tm', 'rows'), may hold values from -12 to 12
- weight: bfloat16 [3, 3, 3, 256, 256], replicated, may hold values from -0.078125 to 0.078125
- bias: float32 [256], replicated, may hold values from -1 to 1
- head: float32 [256], replicated, may hold values from -4 to 4
Outputs:
- grad_weight: float32 [3, 3, 3, 256, 256], replicated
- grad_bias: float32 [256], replicated
- grad_head: float32 [256], replicated
The draws below stay inside these ranges and needn't reach their ends.
All inputs are finite; a program needn't handle non-finite values.
Results may differ from the reference program's by a relative error of at most 0.0003.
Values may be sent and summed in bfloat16 or wider, within the bound.
No kernel may reach another device: no remote copies, remote signals or barrier semaphores. Data moves between devices by JAX's collectives and lax.ppermute only.
A program may use at most 128 MiB of HBM per device.

```python
import jax
import jax.numpy as jnp
from jax import lax

C = 256
WID = 128
NT = 64
NH = 4
CLIPS = 2


def draw_clips(key, part):
    shape = (CLIPS, NT, NH, WID, C)
    frame_scale = 3.0 ** (jnp.arange(NT, dtype=jnp.float32) / max(NT - 1, 1))
    values = jnp.clip(jax.random.normal(key, shape, jnp.float32), -4.0, 4.0)
    return (values * frame_scale[None, :, None, None, None]).astype(jnp.bfloat16)


def centred(key, shape, width, most, kind=jnp.bfloat16):
    return jnp.clip(width * jax.random.normal(key, shape, jnp.float32), -most, most).astype(kind)


def setup_inputs(seed: int = 0) -> dict:
    seeds = jax.random.split(jax.random.key(seed), 5)
    return {
        "clips": draw_clips(jax.random.fold_in(seeds[4], 71), 0),
        "weight": centred(seeds[1], (3, 3, 3, C, C), (27 * C) ** -0.5, 0.078125),
        "bias": jnp.clip(jax.random.uniform(seeds[2], (C,), jnp.float32, -1.0, 1.0), -1.0, 1.0),
        "head": centred(seeds[3], (C,), 1.0, 4.0, jnp.float32),
    }


penalty_weight = 0.01


def conv_offsets(padded, weight, transpose):
    nclip, tpad, rpad, wpad, chans = padded.shape
    frames, rowsn, cols = tpad - 2, rpad - 2, wpad - 2
    total = jnp.zeros((nclip * frames * rowsn * cols, weight.shape[4]), jnp.float32)
    for a in range(3):
        for b in range(3):
            for d in range(3):
                if transpose:
                    piece = padded[:, 2 - a:2 - a + frames, 2 - b:2 - b + rowsn, 2 - d:2 - d + cols]
                    total = total + lax.dot_general(piece.reshape(-1, chans), weight[a, b, d], (((1,), (1,)), ((), ())), preferred_element_type=jnp.float32)
                else:
                    piece = padded[:, a:a + frames, b:b + rowsn, d:d + cols]
                    total = total + jnp.dot(piece.reshape(-1, chans), weight[a, b, d], preferred_element_type=jnp.float32)
    return total.reshape(nclip, frames, rowsn, cols, -1)


def correlate(padded, right):
    nclip, tpad, rpad, wpad, chans = padded.shape
    frames, rowsn, cols = tpad - 2, rpad - 2, wpad - 2
    right_rows = right.reshape(-1, right.shape[-1])
    blocks = []
    for a in range(3):
        for b in range(3):
            for d in range(3):
                piece = padded[:, a:a + frames, b:b + rowsn, d:d + cols].reshape(-1, chans)
                blocks.append(lax.dot_general(piece, right_rows, (((0,), (0,)), ((), ())), preferred_element_type=jnp.float32))
    return jnp.stack(blocks).reshape(3, 3, 3, chans, right.shape[-1])


def pad_all(field):
    return jnp.pad(field, ((0, 0), (1, 1), (1, 1), (1, 1), (0, 0)))


def reference(clips, weight, bias, head):
    clip_pad = pad_all(clips)
    pre = conv_offsets(clip_pad, weight, False) + bias
    sig = jax.nn.sigmoid(pre)
    slope = sig * (1.0 + pre * (1.0 - sig))
    curve = sig * (1.0 - sig) * (2.0 + pre * (1.0 - 2.0 * sig))
    score_grad = (head * slope).astype(jnp.bfloat16)
    input_grad = conv_offsets(pad_all(score_grad), weight, True).astype(jnp.bfloat16)
    grad_pad = pad_all(input_grad)
    back_grad = penalty_weight * conv_offsets(grad_pad, weight, False)
    pre_grad = back_grad * head * curve
    pre_grad_b = pre_grad.astype(jnp.bfloat16)
    grad_weight = penalty_weight * correlate(grad_pad, score_grad) + correlate(clip_pad, pre_grad_b)
    grad_bias = jnp.sum(pre_grad, axis=(0, 1, 2, 3))
    grad_head = jnp.sum(back_grad * slope, axis=(0, 1, 2, 3))
    return grad_weight, grad_bias, grad_head
```

```python
import functools

import jax
import jax.numpy as jnp
from jax import lax
from jax.experimental import pallas as pl
from jax.experimental.pallas import tpu as pltpu
from jax.sharding import Mesh, PartitionSpec as P

PENALTY = 0.01
F32 = jnp.float32
BF16 = jnp.bfloat16
ROWS = 4
COLS = 128
CH = 256
PART = CH // ROWS
TILES = 27 * PART // 8
PIECE = 7
PIECES = 32
ALL = ("yh", "z", "yl", "c", "x")
PLANE = ("yh", "z", "yl")
CHAIN = ("z", "yl", "c")


def moved(fn):
    pairs = []
    for yh in range(2):
        for z in range(8):
            for yl in range(2):
                for c in range(2):
                    for x in range(4):
                        y2, z2, c2, x2 = fn(yh * 2 + yl, z, c, x)
                        y2, z2, x2 = y2 % 4, z2 % 8, x2 % 4
                        src = (((yh * 8 + z) * 2 + yl) * 2 + c) * 4 + x
                        dst = ((((y2 // 2) * 8 + z2) * 2 + y2 % 2) * 2 + c2) * 4 + x2
                        pairs.append((src, dst))
    return pairs


def permute(value, fn):
    return lax.ppermute(value, ALL, moved(fn))


def along_x(step):
    return lambda y, z, c, x: (y, z, c, x + step)


def swap_core(y, z, c, x):
    return (y, z, 1 - c, x)


def split_first(step):
    return lambda y, z, c, x: (y, z, c, x + step) if c else (y + step, z, c, x)


def split_second(step):
    return lambda y, z, c, x: (y + step, z, c, x) if c else (y, z, c, x + step)


def chain(value, step):
    count = 32
    pairs = [(i, i + step) for i in range(count) if 0 <= i + step < count]
    return lax.ppermute(value, CHAIN, pairs)


VMEM = pl.BlockSpec(memory_space=pltpu.VMEM)
SMEM = pl.BlockSpec(memory_space=pltpu.SMEM)
ANY = pl.BlockSpec(memory_space=pl.ANY)


def params(limit=60 << 20):
    return pltpu.CompilerParams(vmem_limit_bytes=limit)


def cost(flops, nbytes):
    return pl.CostEstimate(flops=int(flops), bytes_accessed=int(nbytes), transcendentals=0)


def gather_rows_kernel(pos_ref, own, below, above, across, first, second):
    x = pos_ref[0]
    for shift, ref in ((0, own), (3, below), (1, above), (2, across)):
        row = lax.rem(x + shift, 4)
        first[row] = ref[0]
        second[row] = ref[1]


def gather_rows(pos, own, below, above, across):
    out = jax.ShapeDtypeStruct((ROWS, COLS, CH), BF16)
    return pl.pallas_call(
        gather_rows_kernel,
        out_shape=(out, out),
        in_specs=[SMEM] + [VMEM] * 4,
        out_specs=(VMEM, VMEM),
        compiler_params=params(),
        cost_estimate=cost(1e6, 1 << 20),
        name="gather_rows",
    )(pos, own, below, above, across)


def spread_columns(frames, spread):
    row = lax.broadcasted_iota(jnp.int32, (COLS, CH), 0)
    for f, ref in enumerate(frames):
        for r in range(ROWS):
            slab = ref[r]
            wide = slab.astype(F32)
            left = jnp.where(row == 0, 0.0, pltpu.roll(wide, 1, axis=0))
            right = jnp.where(row == COLS - 1, 0.0, pltpu.roll(wide, COLS - 1, axis=0))
            spread[f, r, :, 0:CH] = left.astype(BF16)
            spread[f, r, :, CH : 2 * CH] = slab
            spread[f, r, :, 2 * CH : 3 * CH] = right.astype(BF16)


TAPS = [(1, 1), (0, 1), (2, 1), (0, 0), (1, 0), (2, 0), (0, 2), (1, 2), (2, 2)]


def start_weights(w_hbm, w_buf, sems):
    for n, (a, b) in enumerate(TAPS):
        pltpu.make_async_copy(w_hbm.at[a, b], w_buf.at[n], sems.at[n]).start()


def convolve(spread, w_hbm, w_buf, sems, acc):
    for n, (a, b) in enumerate(TAPS):
        pltpu.make_async_copy(w_hbm.at[a, b], w_buf.at[n], sems.at[n]).wait()
        rows = ROWS if b == 1 else ROWS - 1
        src = 1 if b == 2 else 0
        dst = 1 if b == 0 else 0
        piece = spread[a : a + 2, src : src + rows].reshape(2 * rows * COLS, 3 * CH)
        term = jnp.dot(piece, w_buf[n], preferred_element_type=F32)
        term = term.reshape(2, rows, COLS, CH)
        if n == 0:
            acc[...] = term
        else:
            acc[:, dst : dst + rows] += term


def forward_kernel(prev, first, second, follow, w_hbm, bias, head, pre, g0, g1, spread, w_buf, sems):
    start_weights(w_hbm, w_buf, sems)
    spread_columns((prev, first, second, follow), spread)
    convolve(spread, w_hbm, w_buf, sems, pre)
    for f, out in ((0, g0), (1, g1)):
        for r in range(ROWS):
            value = pre[f, r] + bias[...]
            pre[f, r] = value
            sig = jax.nn.sigmoid(value)
            slope = sig * (1.0 + value * (1.0 - sig))
            out[r] = (head[...] * slope).astype(BF16)


def transpose_kernel(prev, first, second, follow, w_hbm, g0, g1, spread, acc, w_buf, sems):
    start_weights(w_hbm, w_buf, sems)
    spread_columns((prev, first, second, follow), spread)
    convolve(spread, w_hbm, w_buf, sems, acc)
    for f, out in ((0, g0), (1, g1)):
        out[...] = acc[f].astype(BF16)


def conv_scratch():
    return dict(
        spread=pltpu.VMEM((4, ROWS, COLS, 3 * CH), BF16),
        acc=pltpu.VMEM((2, ROWS, COLS, CH), F32),
        w_buf=pltpu.VMEM((9, 3 * CH, CH), BF16),
        sems=pltpu.SemaphoreType.DMA((9,)),
    )


FRAME = jax.ShapeDtypeStruct((ROWS, COLS, CH), BF16)
CONV_FLOPS = 2 * 1024 * 27 * CH * CH


def forward(frames, w9, bias, head):
    s = conv_scratch()
    return pl.pallas_call(
        forward_kernel,
        out_shape=(jax.ShapeDtypeStruct((2, ROWS, COLS, CH), F32), FRAME, FRAME),
        in_specs=[VMEM] * 4 + [ANY, VMEM, VMEM],
        out_specs=(VMEM, VMEM, VMEM),
        scratch_shapes=[s["spread"], s["w_buf"], s["sems"]],
        compiler_params=params(),
        cost_estimate=cost(CONV_FLOPS, 6 << 20),
        name="forward",
    )(*frames, w9, bias, head)


def transposed(frames, w9):
    s = conv_scratch()
    return pl.pallas_call(
        transpose_kernel,
        out_shape=(FRAME, FRAME),
        in_specs=[VMEM] * 4 + [ANY],
        out_specs=(VMEM, VMEM),
        scratch_shapes=[s["spread"], s["acc"], s["w_buf"], s["sems"]],
        compiler_params=params(),
        cost_estimate=cost(CONV_FLOPS, 5 << 20),
        name="transposed",
    )(*frames, w9)


def part_transposed(frames, x, turned):
    chan = lax.broadcasted_iota(jnp.int32, (PART, CH), 1)
    want = lax.broadcasted_iota(jnp.int32, (PART, CH), 0) + x * PART
    pick = jnp.where(chan == want, 1.0, 0.0).astype(BF16)
    width = ROWS * COLS
    lane = lax.rem(lax.broadcasted_iota(jnp.int32, (PART, width), 1), COLS)
    for f, ref in enumerate(frames):
        flat = ref[...].reshape(width, CH)
        mid = lax.dot_general(pick, flat, (((1,), (1,)), ((), ())), preferred_element_type=F32)
        left = jnp.where(lane == 0, 0.0, pltpu.roll(mid, 1, axis=1))
        right = jnp.where(lane == COLS - 1, 0.0, pltpu.roll(mid, width - 1, axis=1))
        at = slice(f * width, (f + 1) * width)
        turned[0:PART, at] = left.astype(BF16)
        turned[PART : 2 * PART, at] = mid.astype(BF16)
        turned[2 * PART : 3 * PART, at] = right.astype(BF16)


def correlate(turned, grads, b):
    width = ROWS * COLS
    rows = ROWS if b == 1 else ROWS - 1
    src = 1 if b == 2 else 0
    dst = 1 if b == 0 else 0
    left = []
    for a in range(3):
        parts = []
        for f in range(2):
            at = (a + f) * width + src * COLS
            parts.append(turned[:, at : at + rows * COLS])
        left.append(jnp.concatenate(parts, axis=1))
    left = jnp.concatenate(left, axis=0)
    right = [g[dst : dst + rows].reshape(rows * COLS, CH) for g in grads]
    return jnp.dot(left, jnp.concatenate(right, axis=0), preferred_element_type=F32)


def backward_kernel(
    pos, i0, i1, i2, i3, c0, c1, c2, c3, s0, s1, pre, w_hbm, head, out,
    spread, acc, w_buf, turn_i, turn_c, pgb, sems,
):
    x = pos[0]
    core = pos[1]
    start_weights(w_hbm, w_buf, sems)
    grads = (i0, i1, i2, i3)
    spread_columns(grads, spread)
    part_transposed(grads, x, turn_i)
    part_transposed((c0, c1, c2, c3), x, turn_c)
    convolve(spread, w_hbm, w_buf, sems, acc)
    sum_bias = jnp.zeros((8, CH), F32)
    sum_head = jnp.zeros((8, CH), F32)
    for f in range(2):
        for r in range(ROWS):
            back = PENALTY * acc[f, r]
            value = pre[f, r]
            sig = jax.nn.sigmoid(value)
            slope = sig * (1.0 + value * (1.0 - sig))
            curve = sig * (1.0 - sig) * (2.0 + value * (1.0 - 2.0 * sig))
            grad = back * head[...] * curve
            pgb[f, r] = grad.astype(BF16)
            sum_bias = sum_bias + jnp.sum(grad.reshape(COLS // 8, 8, CH), axis=0)
            sum_head = sum_head + jnp.sum((back * slope).reshape(COLS // 8, 8, CH), axis=0)
    total_bias = jnp.sum(sum_bias, axis=0, keepdims=True)
    total_head = jnp.sum(sum_head, axis=0, keepdims=True)
    row = lax.broadcasted_iota(jnp.int32, (8, CH), 0)
    small = jnp.where(row == 0, total_bias, jnp.where(row == 1, total_head, 0.0))
    slots = [jnp.where(core == h, 1, 0) for h in range(2)]
    for b in range(3):
        block = PENALTY * correlate(turn_i, (s0, s1), b) + correlate(turn_c, (pgb.at[0], pgb.at[1]), b)
        for a in range(3):
            for d in range(3):
                k = (a * 3 + b) * 3 + d
                tap = block[(a * 3 + d) * PART : (a * 3 + d + 1) * PART]
                for h in range(2):
                    half = tap[:, h * 128 : (h + 1) * 128].reshape(PART // 8, 8, 128)
                    out[slots[h], k * 8 : (k + 1) * 8] = half
    for h in range(2):
        out[slots[h], TILES] = small[:, h * 128 : (h + 1) * 128]
        out[slots[h], TILES + 1 :] = jnp.zeros((PIECE * PIECES - TILES - 1, 8, 128), F32)


def backward(pos, grads, clips, score, pre, w9, head):
    s = conv_scratch()
    return pl.pallas_call(
        backward_kernel,
        out_shape=jax.ShapeDtypeStruct((2, PIECE * PIECES, 8, 128), F32),
        in_specs=[SMEM] + [VMEM] * 11 + [ANY, VMEM],
        out_specs=VMEM,
        scratch_shapes=[
            s["spread"],
            s["acc"],
            s["w_buf"],
            pltpu.VMEM((3 * PART, 4 * ROWS * COLS), BF16),
            pltpu.VMEM((3 * PART, 4 * ROWS * COLS), BF16),
            pltpu.VMEM((2, ROWS, COLS, CH), BF16),
            s["sems"],
        ],
        compiler_params=params(),
        cost_estimate=cost(CONV_FLOPS * 1.6, 10 << 20),
        name="backward",
    )(pos, *grads, *clips, *score, pre, w9, head)


def relative(distance):
    return jnp.where(distance == 0, 0, jnp.where(distance == 3, 1, distance + 1))


def assemble_kernel(pos, mine, other, out, small):
    x, core, y = pos[0], pos[1], pos[2]
    part = pl.program_id(0)
    at_x = relative(lax.rem(part - x + 4, 4))
    for ref, held in ((mine, core), (other, 1 - core)):
        lane = pl.ds(pl.multiple_of(held * 128, 128), 128)
        for row in range(4):
            at_y = relative(lax.rem(row - y + 4, 4))
            place = jnp.where(held == 0, at_x * 4 + at_y, at_y * 4 + at_x)
            for z in range(8):
                piece = ((row // 2) * 8 + z) * 2 + row % 2
                for j in range(PIECE):
                    tile = piece * PIECE + j
                    if tile < TILES:
                        out[tile // 8, 0, tile % 8, :, lane] = ref[place, z, j]
                    elif tile == TILES:
                        small[:, lane] = ref[place, z, j]


def assemble(pos, mine, other):
    whole = pl.BlockSpec((16, 8, PIECE, 8, 128), lambda i: (0, 0, 0, 0, 0))
    return pl.pallas_call(
        assemble_kernel,
        grid=(ROWS,),
        out_shape=(
            jax.ShapeDtypeStruct((27, ROWS, 8, 8, CH), F32),
            jax.ShapeDtypeStruct((8, CH), F32),
        ),
        in_specs=[SMEM, VMEM, VMEM],
        out_specs=(
            pl.BlockSpec((27, 1, 8, 8, CH), lambda i: (0, i, 0, 0, 0)),
            pl.BlockSpec((8, CH), lambda i: (0, 0)),
        ),
        compiler_params=params(),
        cost_estimate=cost(1e6, 15 << 20),
        name="assemble",
    )(pos, mine, other)


def ring_gather(value, plan):
    below = permute(value, plan(1))
    above = permute(value, plan(-1))
    half = value.shape[0] // 2
    across_low = permute(below[:half], plan(1))
    across_high = permute(above[half:], plan(-1))
    across = jnp.concatenate([across_low, across_high], axis=0)
    return jnp.stack([value, below, above, across])


def per_device(clips, weight, bias, head):
    x = lax.axis_index("x")
    core = lax.axis_index("c")
    y = lax.axis_index("yh") * 2 + lax.axis_index("yl")
    pos = jnp.stack([x, core, y]).astype(jnp.int32)
    own = clips.reshape(2, COLS, CH)
    below = permute(own, along_x(1))
    above = permute(own, along_x(-1))
    across = permute(own, along_x(2))
    w9 = weight.reshape(3, 3, 3 * CH, CH)
    turned = weight[::-1, ::-1, ::-1].swapaxes(3, 4).reshape(3, 3, 3 * CH, CH)
    bias = bias.reshape(1, CH)
    head = head.reshape(1, CH)

    def with_halo(first, second):
        return (chain(second, 1), first, second, chain(first, -1))

    clip_frames = with_halo(*gather_rows(pos, own, below, above, across))
    pre, s0, s1 = forward(clip_frames, w9, bias, head)
    grad_frames = with_halo(*transposed(with_halo(s0, s1), turned))
    terms = backward(pos, grad_frames, clip_frames, (s0, s1), pre, w9, head)
    half = terms[1] + permute(terms[0], swap_core)
    pieces = lax.all_to_all(half.reshape(PIECES, PIECE, 8, 128), PLANE, 0, 0, tiled=True)
    piece = jnp.sum(pieces, axis=0)
    line = jnp.broadcast_to(piece[None], (8, PIECE, 8, 128))
    line = lax.all_to_all(line, "z", 0, 0, tiled=True)
    block = ring_gather(line, split_first)
    mine = ring_gather(block.reshape(32, PIECE, 8, 128), split_second)
    mine = mine.reshape(16, 8, PIECE, 8, 128)
    other = permute(mine, swap_core)
    grad_weight, small = assemble(pos, mine, other)
    return grad_weight.reshape(3, 3, 3, CH, CH), small[0], small[1]


def solution(mesh):
    fine = Mesh(mesh.devices.reshape(2, 8, 2, 2, 4), ALL)
    return jax.shard_map(
        per_device,
        mesh=fine,
        in_specs=(P("yh", CHAIN, "x", None, None), P(), P(), P()),
        out_specs=(P(), P(), P()),
        check_vma=False,
    )
```

```python
import functools

import jax
import jax.numpy as jnp
from jax import lax
from jax.experimental import pallas as pl
from jax.experimental.pallas import tpu as pltpu
from jax.sharding import Mesh, PartitionSpec as P

PENALTY = 0.01
F32 = jnp.float32
BF16 = jnp.bfloat16
ROWS = 4
COLS = 128
CH = 256
PART = CH // ROWS
TILES = 27 * PART // 8
PIECE = 7
PIECES = 32
ALL = ("yh", "z", "yl", "c", "x")
CHAIN = ("z", "yl", "c")


def moved(fn):
    pairs = []
    for yh in range(2):
        for z in range(8):
            for yl in range(2):
                for c in range(2):
                    for x in range(4):
                        y2, z2, c2, x2 = fn(yh * 2 + yl, z, c, x)
                        y2, z2, x2 = y2 % 4, z2 % 8, x2 % 4
                        src = (((yh * 8 + z) * 2 + yl) * 2 + c) * 4 + x
                        dst = ((((y2 // 2) * 8 + z2) * 2 + y2 % 2) * 2 + c2) * 4 + x2
                        pairs.append((src, dst))
    return pairs


def permute(value, fn):
    return lax.ppermute(value, ALL, moved(fn))


def along_x(step):
    return lambda y, z, c, x: (y, z, c, x + step)


def swap_core(y, z, c, x):
    return (y, z, 1 - c, x)


def split_first(step):
    return lambda y, z, c, x: (y, z, c, x + step) if c else (y + step, z, c, x)


def split_second(step):
    return lambda y, z, c, x: (y + step, z, c, x) if c else (y, z, c, x + step)


def chain(value, step):
    count = 32
    pairs = [(i, i + step) for i in range(count) if 0 <= i + step < count]
    return lax.ppermute(value, CHAIN, pairs)


VMEM = pl.BlockSpec(memory_space=pltpu.VMEM)
SMEM = pl.BlockSpec(memory_space=pltpu.SMEM)


def params(limit=24 << 20):
    return pltpu.CompilerParams(vmem_limit_bytes=limit)


def cost(flops, nbytes):
    return pl.CostEstimate(flops=int(flops), bytes_accessed=int(nbytes), transcendentals=0)


def gather_rows_kernel(pos_ref, own, below, above, across, first, second):
    x = pos_ref[0]
    for shift, ref in ((0, own), (3, below), (1, above), (2, across)):
        row = lax.rem(x + shift, 4)
        first[row] = ref[0]
        second[row] = ref[1]


def gather_rows(pos, own, below, above, across):
    out = jax.ShapeDtypeStruct((ROWS, COLS, CH), BF16)
    return pl.pallas_call(
        gather_rows_kernel,
        out_shape=(out, out),
        in_specs=[SMEM] + [VMEM] * 4,
        out_specs=(VMEM, VMEM),
        compiler_params=params(),
        cost_estimate=cost(1e6, 1 << 20),
        name="gather_rows",
    )(pos, own, below, above, across)


def spread_columns(frames, spread):
    row = lax.broadcasted_iota(jnp.int32, (COLS, CH), 0)
    for f, ref in enumerate(frames):
        for r in range(ROWS):
            slab = ref[r]
            wide = slab.astype(F32)
            left = jnp.where(row == 0, 0.0, pltpu.roll(wide, 1, axis=0))
            right = jnp.where(row == COLS - 1, 0.0, pltpu.roll(wide, COLS - 1, axis=0))
            spread[f, r, :, 0:CH] = left.astype(BF16)
            spread[f, r, :, CH : 2 * CH] = slab
            spread[f, r, :, 2 * CH : 3 * CH] = right.astype(BF16)


TAPS = [(1, 1), (0, 1), (2, 1), (0, 0), (1, 0), (2, 0), (0, 2), (1, 2), (2, 2)]


def convolve(spread, weight, acc):
    for n, (a, b) in enumerate(TAPS):
        rows = ROWS if b == 1 else ROWS - 1
        src = 1 if b == 2 else 0
        dst = 1 if b == 0 else 0
        piece = spread[a : a + 2, src : src + rows].reshape(2 * rows * COLS, 3 * CH)
        term = jnp.dot(piece, weight[a, b], preferred_element_type=F32)
        term = term.reshape(2, rows, COLS, CH)
        if n == 0:
            acc[...] = term
        else:
            acc[:, dst : dst + rows] += term


def forward_kernel(prev, first, second, follow, weight, bias, head, pre, g0, g1, spread):
    spread_columns((prev, first, second, follow), spread)
    convolve(spread, weight, pre)
    for f, out in ((0, g0), (1, g1)):
        for r in range(ROWS):
            value = pre[f, r] + bias[...]
            pre[f, r] = value
            sig = jax.nn.sigmoid(value)
            slope = sig * (1.0 + value * (1.0 - sig))
            out[r] = (head[...] * slope).astype(BF16)


def transpose_kernel(prev, first, second, follow, weight, g0, g1, spread, acc):
    spread_columns((prev, first, second, follow), spread)
    convolve(spread, weight, acc)
    for f, out in ((0, g0), (1, g1)):
        out[...] = acc[f].astype(BF16)


def conv_scratch():
    return dict(
        spread=pltpu.VMEM((4, ROWS, COLS, 3 * CH), BF16),
        acc=pltpu.VMEM((2, ROWS, COLS, CH), F32),
    )


def turn_kernel(weight, out):
    for d in range(3):
        out[0, 0, 2 - d] = weight[0, 0, d].T


def turn_weights(weight):
    return pl.pallas_call(
        turn_kernel,
        grid=(9,),
        out_shape=jax.ShapeDtypeStruct((3, 3, 3, CH, CH), BF16),
        in_specs=[pl.BlockSpec((1, 1, 3, CH, CH), lambda n: (n // 3, n % 3, 0, 0, 0))],
        out_specs=pl.BlockSpec((1, 1, 3, CH, CH), lambda n: (2 - n // 3, 2 - n % 3, 0, 0, 0)),
        compiler_params=params(8 << 20),
        cost_estimate=cost(2e9, 8 << 20),
        name="turn_weights",
    )(weight)


FRAME = jax.ShapeDtypeStruct((ROWS, COLS, CH), BF16)
CONV_FLOPS = 2 * 1024 * 27 * CH * CH


def forward(frames, w9, bias, head):
    s = conv_scratch()
    return pl.pallas_call(
        forward_kernel,
        out_shape=(jax.ShapeDtypeStruct((2, ROWS, COLS, CH), F32), FRAME, FRAME),
        in_specs=[VMEM] * 7,
        out_specs=(VMEM, VMEM, VMEM),
        scratch_shapes=[s["spread"]],
        compiler_params=params(),
        cost_estimate=cost(CONV_FLOPS, 6 << 20),
        name="forward",
    )(*frames, w9, bias, head)


def transposed(frames, w9):
    s = conv_scratch()
    return pl.pallas_call(
        transpose_kernel,
        out_shape=(FRAME, FRAME),
        in_specs=[VMEM] * 5,
        out_specs=(VMEM, VMEM),
        scratch_shapes=[s["spread"], s["acc"]],
        compiler_params=params(),
        cost_estimate=cost(CONV_FLOPS, 5 << 20),
        name="transposed",
    )(*frames, w9)


def part_transposed(frames, x, turned):
    chan = lax.broadcasted_iota(jnp.int32, (PART, CH), 1)
    want = lax.broadcasted_iota(jnp.int32, (PART, CH), 0) + x * PART
    pick = jnp.where(chan == want, 1.0, 0.0).astype(BF16)
    width = ROWS * COLS
    lane = lax.rem(lax.broadcasted_iota(jnp.int32, (PART, width), 1), COLS)
    for f, ref in enumerate(frames):
        flat = ref[...].reshape(width, CH)
        mid = lax.dot_general(pick, flat, (((1,), (1,)), ((), ())), preferred_element_type=F32)
        left = jnp.where(lane == 0, 0.0, pltpu.roll(mid, 1, axis=1))
        right = jnp.where(lane == COLS - 1, 0.0, pltpu.roll(mid, width - 1, axis=1))
        at = slice(f * width, (f + 1) * width)
        turned[0:PART, at] = left.astype(BF16)
        turned[PART : 2 * PART, at] = mid.astype(BF16)
        turned[2 * PART : 3 * PART, at] = right.astype(BF16)


def correlate(turned, grads, b):
    width = ROWS * COLS
    rows = ROWS if b == 1 else ROWS - 1
    src = 1 if b == 2 else 0
    dst = 1 if b == 0 else 0
    left = []
    for a in range(3):
        parts = []
        for f in range(2):
            at = (a + f) * width + src * COLS
            parts.append(turned[:, at : at + rows * COLS])
        left.append(jnp.concatenate(parts, axis=1))
    left = jnp.concatenate(left, axis=0)
    right = [g[dst : dst + rows].reshape(rows * COLS, CH) for g in grads]
    return jnp.dot(left, jnp.concatenate(right, axis=0), preferred_element_type=F32)


def backward_kernel(
    pos, i0, i1, i2, i3, c0, c1, c2, c3, s0, s1, pre, weight, head, sent, kept,
    spread, acc, turn_i, turn_c, pgb, total,
):
    x = pos[0]
    core = pos[1]
    grads = (i0, i1, i2, i3)
    spread_columns(grads, spread)
    part_transposed(grads, x, turn_i)
    part_transposed((c0, c1, c2, c3), x, turn_c)
    convolve(spread, weight, acc)
    sum_bias = jnp.zeros((8, CH), F32)
    sum_head = jnp.zeros((8, CH), F32)
    for f in range(2):
        for r in range(ROWS):
            back = PENALTY * acc[f, r]
            value = pre[f, r]
            sig = jax.nn.sigmoid(value)
            slope = sig * (1.0 + value * (1.0 - sig))
            curve = sig * (1.0 - sig) * (2.0 + value * (1.0 - 2.0 * sig))
            grad = back * head[...] * curve
            pgb[f, r] = grad.astype(BF16)
            sum_bias = sum_bias + jnp.sum(grad.reshape(COLS // 8, 8, CH), axis=0)
            sum_head = sum_head + jnp.sum((back * slope).reshape(COLS // 8, 8, CH), axis=0)
    total_bias = jnp.sum(sum_bias, axis=0, keepdims=True)
    total_head = jnp.sum(sum_head, axis=0, keepdims=True)
    row = lax.broadcasted_iota(jnp.int32, (8, CH), 0)
    small = jnp.where(row == 0, total_bias, jnp.where(row == 1, total_head, 0.0))
    blocks = []
    for b in range(3):
        block = PENALTY * correlate(turn_i, (s0, s1), b) + correlate(turn_c, (pgb.at[0], pgb.at[1]), b)
        blocks.append(block)
    for b, block in enumerate(blocks):
        total[b * 9 * PART : (b + 1) * 9 * PART] = block

    def store(out, h):
        lanes = slice(h * 128, (h + 1) * 128)
        for k in range(27):
            a, b, d = k // 9, (k // 3) % 3, k % 3
            at = ((b * 3 + a) * 3 + d) * PART
            out[k * 8 : (k + 1) * 8] = total[at : at + PART, lanes].reshape(PART // 8, 8, 128)
        out[TILES] = small[:, lanes]
        out[TILES + 1 :] = jnp.zeros((PIECE * PIECES - TILES - 1, 8, 128), F32)

    @pl.when(core == 0)
    def _():
        store(kept, 0)
        store(sent, 1)

    @pl.when(core == 1)
    def _():
        store(kept, 1)
        store(sent, 0)


def backward(pos, grads, clips, score, pre, w9, head):
    s = conv_scratch()
    return pl.pallas_call(
        backward_kernel,
        out_shape=(jax.ShapeDtypeStruct((PIECE * PIECES, 8, 128), F32),) * 2,
        in_specs=[SMEM] + [VMEM] * 13,
        out_specs=(VMEM, VMEM),
        scratch_shapes=[
            s["spread"],
            s["acc"],
            pltpu.VMEM((3 * PART, 4 * ROWS * COLS), BF16),
            pltpu.VMEM((3 * PART, 4 * ROWS * COLS), BF16),
            pltpu.VMEM((2, ROWS, COLS, CH), BF16),
            pltpu.VMEM((27 * PART, CH), F32),
        ],
        compiler_params=params(),
        cost_estimate=cost(CONV_FLOPS * 1.6, 10 << 20),
        name="backward",
    )(pos, *grads, *clips, *score, pre, w9, head)


def relative(distance):
    return jnp.where(distance == 0, 0, jnp.where(distance == 3, 1, distance + 1))


def assemble_kernel(pos, mine, other, out, small):
    x, core, y = pos[0], pos[1], pos[2]
    part = pl.program_id(0)
    at_x = relative(lax.rem(part - x + 4, 4))
    for ref, held in ((mine, core), (other, 1 - core)):
        lane = pl.ds(pl.multiple_of(held * 128, 128), 128)
        for row in range(4):
            at_y = relative(lax.rem(row - y + 4, 4))
            place = jnp.where(held == 0, at_x * 4 + at_y, at_y * 4 + at_x)
            for z in range(8):
                piece = row * 8 + z
                for j in range(PIECE):
                    tile = piece * PIECE + j
                    if tile < TILES:
                        out[tile // 8, 0, tile % 8, :, lane] = ref[place, z, j]
                    elif tile == TILES:
                        small[:, lane] = ref[place, z, j]


def assemble(pos, mine, other):
    whole = pl.BlockSpec((16, 8, PIECE, 8, 128), lambda i: (0, 0, 0, 0, 0))
    return pl.pallas_call(
        assemble_kernel,
        grid=(ROWS,),
        out_shape=(
            jax.ShapeDtypeStruct((27, ROWS, 8, 8, CH), F32),
            jax.ShapeDtypeStruct((8, CH), F32),
        ),
        in_specs=[SMEM, VMEM, VMEM],
        out_specs=(
            pl.BlockSpec((27, 1, 8, 8, CH), lambda i: (0, i, 0, 0, 0)),
            pl.BlockSpec((8, CH), lambda i: (0, 0)),
        ),
        compiler_params=params(),
        cost_estimate=cost(1e6, 15 << 20),
        name="assemble",
    )(pos, mine, other)


def ring_gather(value, plan):
    below = permute(value, plan(1))
    above = permute(value, plan(-1))
    half = value.shape[0] // 2
    across_low = permute(below[:half], plan(1))
    across_high = permute(above[half:], plan(-1))
    across = jnp.concatenate([across_low, across_high], axis=0)
    return jnp.stack([value, below, above, across])


def per_device(clips, weight, bias, head):
    x = lax.axis_index("x")
    core = lax.axis_index("c")
    y = lax.axis_index("yh") * 2 + lax.axis_index("yl")
    pos = jnp.stack([x, core, y]).astype(jnp.int32)
    own = clips.reshape(2, COLS, CH)
    below = permute(own, along_x(1))
    above = permute(own, along_x(-1))
    across = permute(own, along_x(2))
    w9 = weight.reshape(3, 3, 3 * CH, CH)
    turned = turn_weights(weight).reshape(3, 3, 3 * CH, CH)
    bias = bias.reshape(1, CH)
    head = head.reshape(1, CH)

    def with_halo(first, second):
        return (chain(second, 1), first, second, chain(first, -1))

    clip_frames = with_halo(*gather_rows(pos, own, below, above, across))
    pre, s0, s1 = forward(clip_frames, w9, bias, head)
    grad_frames = with_halo(*transposed(with_halo(s0, s1), turned))
    sent, kept = backward(pos, grad_frames, clip_frames, (s0, s1), pre, w9, head)
    half = kept + permute(sent, swap_core)
    lines = lax.all_to_all(half.reshape(4, 8, PIECE, 8, 128), ("yh", "yl"), 0, 0, tiled=True)
    line = jnp.sum(lines, axis=0)
    pieces = lax.all_to_all(line, "z", 0, 0, tiled=True)
    piece = jnp.sum(pieces, axis=0)
    line = jnp.broadcast_to(piece[None], (8, PIECE, 8, 128))
    line = lax.all_to_all(line, "z", 0, 0, tiled=True)
    block = ring_gather(line, split_first)
    mine = ring_gather(block.reshape(32, PIECE, 8, 128), split_second)
    mine = mine.reshape(16, 8, PIECE, 8, 128)
    other = permute(mine, swap_core)
    grad_weight, small = assemble(pos, mine, other)
    return grad_weight.reshape(3, 3, 3, CH, CH), small[0], small[1]


def solution(mesh):
    fine = Mesh(mesh.devices.reshape(2, 8, 2, 2, 4), ALL)
    return jax.shard_map(
        per_device,
        mesh=fine,
        in_specs=(P("yh", CHAIN, "x", None, None), P(), P(), P()),
        out_specs=(P(), P(), P()),
        check_vma=False,
    )
```

```python
import functools

import jax
import jax.numpy as jnp
from jax import lax
from jax.experimental import pallas as pl
from jax.experimental.pallas import tpu as pltpu
from jax.sharding import Mesh, PartitionSpec as P

PENALTY = 0.01
F32 = jnp.float32
BF16 = jnp.bfloat16
ROWS = 4
COLS = 128
CH = 256
PART = CH // ROWS
TILES = 27 * PART // 8
PIECE = 7
PIECES = 32
CODED = 64
SPAN = 250.0
ALL = ("yh", "z", "yl", "c", "x")
CHAIN = ("z", "yl", "c")


def moved(fn):
    pairs = []
    for yh in range(2):
        for z in range(8):
            for yl in range(2):
                for c in range(2):
                    for x in range(4):
                        y2, z2, c2, x2 = fn(yh * 2 + yl, z, c, x)
                        y2, z2, x2 = y2 % 4, z2 % 8, x2 % 4
                        src = (((yh * 8 + z) * 2 + yl) * 2 + c) * 4 + x
                        dst = ((((y2 // 2) * 8 + z2) * 2 + y2 % 2) * 2 + c2) * 4 + x2
                        pairs.append((src, dst))
    return pairs


def permute(value, fn):
    return lax.ppermute(value, ALL, moved(fn))


def along_x(step):
    return lambda y, z, c, x: (y, z, c, x + step)


def swap_core(y, z, c, x):
    return (y, z, 1 - c, x)


def split_first(step):
    return lambda y, z, c, x: (y, z, c, x + step) if c else (y + step, z, c, x)


def split_second(step):
    return lambda y, z, c, x: (y + step, z, c, x) if c else (y, z, c, x + step)


def chain(value, step):
    count = 32
    pairs = [(i, i + step) for i in range(count) if 0 <= i + step < count]
    return lax.ppermute(value, CHAIN, pairs)


VMEM = pl.BlockSpec(memory_space=pltpu.VMEM)
SMEM = pl.BlockSpec(memory_space=pltpu.SMEM)


def params(limit=24 << 20):
    return pltpu.CompilerParams(vmem_limit_bytes=limit)


def cost(flops, nbytes):
    return pl.CostEstimate(flops=int(flops), bytes_accessed=int(nbytes), transcendentals=0)


def gather_rows_kernel(pos_ref, own, below, above, across, first, second):
    x = pos_ref[0]
    for shift, ref in ((0, own), (3, below), (1, above), (2, across)):
        row = lax.rem(x + shift, 4)
        first[row] = ref[0]
        second[row] = ref[1]


def gather_rows(pos, own, below, above, across):
    out = jax.ShapeDtypeStruct((ROWS, COLS, CH), BF16)
    return pl.pallas_call(
        gather_rows_kernel,
        out_shape=(out, out),
        in_specs=[SMEM] + [VMEM] * 4,
        out_specs=(VMEM, VMEM),
        compiler_params=params(),
        cost_estimate=cost(1e6, 1 << 20),
        name="gather_rows",
    )(pos, own, below, above, across)


def spread_columns(frames, spread):
    row = lax.broadcasted_iota(jnp.int32, (COLS, CH), 0)
    for f, ref in enumerate(frames):
        for r in range(ROWS):
            slab = ref[r]
            wide = slab.astype(F32)
            left = jnp.where(row == 0, 0.0, pltpu.roll(wide, 1, axis=0))
            right = jnp.where(row == COLS - 1, 0.0, pltpu.roll(wide, COLS - 1, axis=0))
            spread[f, r, :, 0:CH] = left.astype(BF16)
            spread[f, r, :, CH : 2 * CH] = slab
            spread[f, r, :, 2 * CH : 3 * CH] = right.astype(BF16)


TAPS = [(1, 1), (0, 1), (2, 1), (0, 0), (1, 0), (2, 0), (0, 2), (1, 2), (2, 2)]


def convolve(spread, weight, acc):
    for n, (a, b) in enumerate(TAPS):
        rows = ROWS if b == 1 else ROWS - 1
        src = 1 if b == 2 else 0
        dst = 1 if b == 0 else 0
        piece = spread[a : a + 2, src : src + rows].reshape(2 * rows * COLS, 3 * CH)
        term = jnp.dot(piece, weight[a, b], preferred_element_type=F32)
        term = term.reshape(2, rows, COLS, CH)
        if n == 0:
            acc[...] = term
        else:
            acc[:, dst : dst + rows] += term


def forward_kernel(prev, first, second, follow, weight, bias, head, pre, g0, g1, spread):
    spread_columns((prev, first, second, follow), spread)
    convolve(spread, weight, pre)
    for f, out in ((0, g0), (1, g1)):
        for r in range(ROWS):
            value = pre[f, r] + bias[...]
            pre[f, r] = value
            sig = jax.nn.sigmoid(value)
            slope = sig * (1.0 + value * (1.0 - sig))
            out[r] = (head[...] * slope).astype(BF16)


def transpose_kernel(prev, first, second, follow, weight, g0, g1, spread, acc):
    spread_columns((prev, first, second, follow), spread)
    convolve(spread, weight, acc)
    for f, out in ((0, g0), (1, g1)):
        out[...] = acc[f].astype(BF16)


def conv_scratch():
    return dict(
        spread=pltpu.VMEM((4, ROWS, COLS, 3 * CH), BF16),
        acc=pltpu.VMEM((2, ROWS, COLS, CH), F32),
    )


def turn_kernel(weight, bias, head, out, same, bias_out, head_out):
    for d in range(3):
        tap = weight[0, 0, d]
        same[0, 0, d] = tap
        out[0, 0, 2 - d] = tap.T
    bias_out[...] = bias[...]
    head_out[...] = head[...]


def turn_weights(weight, bias, head):
    full = jax.ShapeDtypeStruct((3, 3, 3, CH, CH), BF16)
    row = jax.ShapeDtypeStruct((1, CH), F32)
    here = pl.BlockSpec((1, 1, 3, CH, CH), lambda n: (n // 3, n % 3, 0, 0, 0))
    line = pl.BlockSpec((1, CH), lambda n: (0, 0))
    return pl.pallas_call(
        turn_kernel,
        grid=(9,),
        out_shape=(full, full, row, row),
        in_specs=[here, line, line],
        out_specs=(
            pl.BlockSpec((1, 1, 3, CH, CH), lambda n: (2 - n // 3, 2 - n % 3, 0, 0, 0)),
            here,
            line,
            line,
        ),
        compiler_params=params(8 << 20),
        cost_estimate=cost(2e9, 11 << 20),
        name="turn_weights",
    )(weight, bias, head)


FRAME = jax.ShapeDtypeStruct((ROWS, COLS, CH), BF16)
CONV_FLOPS = 2 * 1024 * 27 * CH * CH


def forward(frames, w9, bias, head):
    s = conv_scratch()
    return pl.pallas_call(
        forward_kernel,
        out_shape=(jax.ShapeDtypeStruct((2, ROWS, COLS, CH), F32), FRAME, FRAME),
        in_specs=[VMEM] * 7,
        out_specs=(VMEM, VMEM, VMEM),
        scratch_shapes=[s["spread"]],
        compiler_params=params(),
        cost_estimate=cost(CONV_FLOPS, 6 << 20),
        name="forward",
    )(*frames, w9, bias, head)


def transposed(frames, w9):
    s = conv_scratch()
    return pl.pallas_call(
        transpose_kernel,
        out_shape=(FRAME, FRAME),
        in_specs=[VMEM] * 5,
        out_specs=(VMEM, VMEM),
        scratch_shapes=[s["spread"], s["acc"]],
        compiler_params=params(),
        cost_estimate=cost(CONV_FLOPS, 5 << 20),
        name="transposed",
    )(*frames, w9)


def part_transposed(frames, x, turned):
    chan = lax.broadcasted_iota(jnp.int32, (PART, CH), 1)
    want = lax.broadcasted_iota(jnp.int32, (PART, CH), 0) + x * PART
    pick = jnp.where(chan == want, 1.0, 0.0).astype(BF16)
    width = ROWS * COLS
    lane = lax.rem(lax.broadcasted_iota(jnp.int32, (PART, width), 1), COLS)
    for f, ref in enumerate(frames):
        flat = ref[...].reshape(width, CH)
        mid = lax.dot_general(pick, flat, (((1,), (1,)), ((), ())), preferred_element_type=F32)
        left = jnp.where(lane == 0, 0.0, pltpu.roll(mid, 1, axis=1))
        right = jnp.where(lane == COLS - 1, 0.0, pltpu.roll(mid, width - 1, axis=1))
        at = slice(f * width, (f + 1) * width)
        turned[0:PART, at] = left.astype(BF16)
        turned[PART : 2 * PART, at] = mid.astype(BF16)
        turned[2 * PART : 3 * PART, at] = right.astype(BF16)


def correlate(turned, grads, b):
    width = ROWS * COLS
    rows = ROWS if b == 1 else ROWS - 1
    src = 1 if b == 2 else 0
    dst = 1 if b == 0 else 0
    left = []
    for a in range(3):
        parts = []
        for f in range(2):
            at = (a + f) * width + src * COLS
            parts.append(turned[:, at : at + rows * COLS])
        left.append(jnp.concatenate(parts, axis=1))
    left = jnp.concatenate(left, axis=0)
    right = [g[dst : dst + rows].reshape(rows * COLS, CH) for g in grads]
    return jnp.dot(left, jnp.concatenate(right, axis=0), preferred_element_type=F32)


def backward_kernel(
    pos, i0, i1, i2, i3, c0, c1, c2, c3, s0, s1, pre, weight, head, sent, kept,
    spread, acc, turn_i, turn_c, pgb, total,
):
    x = pos[0]
    core = pos[1]
    grads = (i0, i1, i2, i3)
    spread_columns(grads, spread)
    part_transposed(grads, x, turn_i)
    part_transposed((c0, c1, c2, c3), x, turn_c)
    convolve(spread, weight, acc)
    sum_bias = jnp.zeros((8, CH), F32)
    sum_head = jnp.zeros((8, CH), F32)
    for f in range(2):
        for r in range(ROWS):
            back = PENALTY * acc[f, r]
            value = pre[f, r]
            sig = jax.nn.sigmoid(value)
            slope = sig * (1.0 + value * (1.0 - sig))
            curve = sig * (1.0 - sig) * (2.0 + value * (1.0 - 2.0 * sig))
            grad = back * head[...] * curve
            pgb[f, r] = grad.astype(BF16)
            sum_bias = sum_bias + jnp.sum(grad.reshape(COLS // 8, 8, CH), axis=0)
            sum_head = sum_head + jnp.sum((back * slope).reshape(COLS // 8, 8, CH), axis=0)
    total_bias = jnp.sum(sum_bias, axis=0, keepdims=True)
    total_head = jnp.sum(sum_head, axis=0, keepdims=True)
    row = lax.broadcasted_iota(jnp.int32, (8, CH), 0)
    small_bias = jnp.where(row == 0, total_bias, 0.0)
    small_head = jnp.where(row == 0, total_head, 0.0)
    blocks = []
    for b in range(3):
        block = PENALTY * correlate(turn_i, (s0, s1), b) + correlate(turn_c, (pgb.at[0], pgb.at[1]), b)
        blocks.append(block)
    for b, block in enumerate(blocks):
        total[b * 9 * PART : (b + 1) * 9 * PART] = block

    def store(out, h):
        lanes = slice(h * 128, (h + 1) * 128)
        for k in range(27):
            a, b, d = k // 9, (k // 3) % 3, k % 3
            at = ((b * 3 + a) * 3 + d) * PART
            out[k * 8 : (k + 1) * 8] = total[at : at + PART, lanes].reshape(PART // 8, 8, 128)
        out[TILES] = small_bias[:, lanes]
        out[TILES + 1] = small_head[:, lanes]
        out[TILES + 2 :] = jnp.zeros((PIECE * PIECES - TILES - 2, 8, 128), F32)

    @pl.when(core == 0)
    def _():
        store(kept, 0)
        store(sent, 1)

    @pl.when(core == 1)
    def _():
        store(kept, 1)
        store(sent, 0)


def backward(pos, grads, clips, score, pre, w9, head):
    s = conv_scratch()
    return pl.pallas_call(
        backward_kernel,
        out_shape=(jax.ShapeDtypeStruct((PIECE * PIECES, 8, 128), F32),) * 2,
        in_specs=[SMEM] + [VMEM] * 13,
        out_specs=(VMEM, VMEM),
        scratch_shapes=[
            s["spread"],
            s["acc"],
            pltpu.VMEM((3 * PART, 4 * ROWS * COLS), BF16),
            pltpu.VMEM((3 * PART, 4 * ROWS * COLS), BF16),
            pltpu.VMEM((2, ROWS, COLS, CH), BF16),
            pltpu.VMEM((27 * PART, CH), F32),
        ],
        compiler_params=params(),
        cost_estimate=cost(CONV_FLOPS * 1.6, 10 << 20),
        name="backward",
    )(pos, *grads, *clips, *score, pre, w9, head)


def relative(distance):
    return jnp.where(distance == 0, 0, jnp.where(distance == 3, 1, distance + 1))


def encode_kernel(terms, out):
    value = terms[0]
    for n in range(1, 8):
        value = value + terms[n]
    most = jnp.max(jnp.abs(value), axis=1, keepdims=True)
    scale = (most * 1.004).astype(BF16)
    wide = scale.astype(F32)
    inverse = jnp.where(wide > 1e-37, 1.0 / jnp.maximum(wide, 1e-37), 0.0)
    code = jnp.exp2(jnp.abs(value) * inverse * SPAN - SPAN / 2)
    code = jnp.where(value < 0, -code, code).reshape(PIECE * 8, 128)
    pad = jnp.zeros((1, 128), F32)
    tail = jnp.concatenate([wide.reshape(PIECE, 128), pad], axis=0)
    line = jnp.concatenate([code, tail], axis=0).astype(BF16)
    for n in range(8):
        out[n] = line


def encode(terms):
    return pl.pallas_call(
        encode_kernel,
        out_shape=jax.ShapeDtypeStruct((8, CODED, 128), BF16),
        in_specs=[VMEM],
        out_specs=VMEM,
        compiler_params=params(4 << 20),
        cost_estimate=cost(1e6, 1 << 19),
        name="encode",
    )(terms)


def decode(line):
    wide = line.astype(F32)
    level = jnp.log2(jnp.abs(wide[: PIECE * 8])) * (1.0 / SPAN) + 0.5
    level = jnp.where(wide[: PIECE * 8] < 0, -level, level)
    return [
        level[8 * j : 8 * j + 8] * wide[PIECE * 8 + j : PIECE * 8 + j + 1] for j in range(PIECE)
    ]


def assemble_kernel(pos, mine, other, out, small):
    x, core, y = pos[0], pos[1], pos[2]
    part = pl.program_id(0)
    at_x = relative(lax.rem(part - x + 4, 4))
    for ref, held in ((mine, core), (other, 1 - core)):
        lane = pl.ds(pl.multiple_of(held * 128, 128), 128)
        for row in range(4):
            at_y = relative(lax.rem(row - y + 4, 4))
            place = jnp.where(held == 0, at_x * 4 + at_y, at_y * 4 + at_x)
            for z in range(8):
                piece = row * 8 + z
                for j, value in enumerate(decode(ref[place, z])):
                    tile = piece * PIECE + j
                    if tile < TILES:
                        out[tile // 8, 0, tile % 8, :, lane] = value
                    elif tile < TILES + 2:
                        at = (tile - TILES) * 8
                        small[at : at + 8, lane] = value


def assemble(pos, mine, other):
    return pl.pallas_call(
        assemble_kernel,
        grid=(ROWS,),
        out_shape=(
            jax.ShapeDtypeStruct((27, ROWS, 8, 8, CH), F32),
            jax.ShapeDtypeStruct((16, CH), F32),
        ),
        in_specs=[SMEM, VMEM, VMEM],
        out_specs=(
            pl.BlockSpec((27, 1, 8, 8, CH), lambda i: (0, i, 0, 0, 0)),
            pl.BlockSpec((16, CH), lambda i: (0, 0)),
        ),
        compiler_params=params(),
        cost_estimate=cost(1e6, 15 << 20),
        name="assemble",
    )(pos, mine, other)


def ring_gather(value, plan):
    below = permute(value, plan(1))
    above = permute(value, plan(-1))
    half = value.shape[0] // 2
    across_low = permute(below[:half], plan(1))
    across_high = permute(above[half:], plan(-1))
    across = jnp.concatenate([across_low, across_high], axis=0)
    return jnp.stack([value, below, above, across])


def per_device(clips, weight, bias, head):
    x = lax.axis_index("x")
    core = lax.axis_index("c")
    y = lax.axis_index("yh") * 2 + lax.axis_index("yl")
    pos = jnp.stack([x, core, y]).astype(jnp.int32)
    own = clips.reshape(2, COLS, CH)
    below = permute(own, along_x(1))
    above = permute(own, along_x(-1))
    across = permute(own, along_x(2))
    turned, weight, bias, head = turn_weights(weight, bias.reshape(1, CH), head.reshape(1, CH))
    turned = turned.reshape(3, 3, 3 * CH, CH)
    w9 = weight.reshape(3, 3, 3 * CH, CH)

    def with_halo(first, second):
        return (chain(second, 1), first, second, chain(first, -1))

    clip_frames = with_halo(*gather_rows(pos, own, below, above, across))
    pre, s0, s1 = forward(clip_frames, w9, bias, head)
    grad_frames = with_halo(*transposed(with_halo(s0, s1), turned))
    sent, kept = backward(pos, grad_frames, clip_frames, (s0, s1), pre, w9, head)
    half = kept + permute(sent, swap_core)
    lines = lax.all_to_all(half.reshape(4, 8, PIECE, 8, 128), ("yh", "yl"), 0, 0, tiled=True)
    line = jnp.sum(lines, axis=0)
    pieces = lax.all_to_all(line, "z", 0, 0, tiled=True)
    line = lax.all_to_all(encode(pieces), "z", 0, 0, tiled=True)
    block = ring_gather(line, split_first)
    mine = ring_gather(block.reshape(32, CODED, 128), split_second)
    mine = mine.reshape(16, 8, CODED, 128)
    other = permute(mine, swap_core)
    grad_weight, small = assemble(pos, mine, other)
    return grad_weight.reshape(3, 3, 3, CH, CH), small[0], small[8]


def solution(mesh):
    fine = Mesh(mesh.devices.reshape(2, 8, 2, 2, 4), ALL)
    return jax.shard_map(
        per_device,
        mesh=fine,
        in_specs=(P("yh", CHAIN, "x", None, None), P(), P(), P()),
        out_specs=(P(), P(), P()),
        check_vma=False,
    )
```

```python
import functools

import jax
import jax.numpy as jnp
from jax import lax
from jax.experimental import pallas as pl
from jax.experimental.pallas import tpu as pltpu
from jax.sharding import Mesh, PartitionSpec as P

PENALTY = 0.01
F32 = jnp.float32
BF16 = jnp.bfloat16
ROWS = 4
COLS = 128
CH = 256
PART = CH // ROWS
TILES = 27 * PART // 8
PIECE = 7
PIECES = 32
CODED = 64
SPAN = 250.0
ALL = ("yh", "z", "yl", "c", "x")
PLANE = ("yh", "z", "yl")
CHAIN = ("z", "yl", "c")


def moved(fn):
    pairs = []
    for yh in range(2):
        for z in range(8):
            for yl in range(2):
                for c in range(2):
                    for x in range(4):
                        y2, z2, c2, x2 = fn(yh * 2 + yl, z, c, x)
                        y2, z2, x2 = y2 % 4, z2 % 8, x2 % 4
                        src = (((yh * 8 + z) * 2 + yl) * 2 + c) * 4 + x
                        dst = ((((y2 // 2) * 8 + z2) * 2 + y2 % 2) * 2 + c2) * 4 + x2
                        pairs.append((src, dst))
    return pairs


def permute(value, fn):
    return lax.ppermute(value, ALL, moved(fn))


def along_x(step):
    return lambda y, z, c, x: (y, z, c, x + step)


def swap_core(y, z, c, x):
    return (y, z, 1 - c, x)


def split_first(step):
    return lambda y, z, c, x: (y, z, c, x + step) if c else (y + step, z, c, x)


def split_second(step):
    return lambda y, z, c, x: (y + step, z, c, x) if c else (y, z, c, x + step)


def chain(value, step):
    count = 32
    pairs = [(i, i + step) for i in range(count) if 0 <= i + step < count]
    return lax.ppermute(value, CHAIN, pairs)


VMEM = pl.BlockSpec(memory_space=pltpu.VMEM)
SMEM = pl.BlockSpec(memory_space=pltpu.SMEM)


def params(limit=24 << 20):
    return pltpu.CompilerParams(vmem_limit_bytes=limit)


def cost(flops, nbytes):
    return pl.CostEstimate(flops=int(flops), bytes_accessed=int(nbytes), transcendentals=0)


def gather_rows_kernel(pos_ref, own, below, above, across, ready, first, second):
    del ready
    x = pos_ref[0]
    for shift, ref in ((0, own), (3, below), (1, above), (2, across)):
        row = lax.rem(x + shift, 4)
        first[row] = ref[0]
        second[row] = ref[1]


def gather_rows(pos, own, below, above, across, ready):
    out = jax.ShapeDtypeStruct((ROWS, COLS, CH), BF16)
    return pl.pallas_call(
        gather_rows_kernel,
        out_shape=(out, out),
        in_specs=[SMEM] + [VMEM] * 5,
        out_specs=(VMEM, VMEM),
        compiler_params=params(),
        cost_estimate=cost(1e6, 1 << 20),
        name="gather_rows",
    )(pos, own, below, above, across, ready)


def spread_columns(frames, spread):
    row = lax.broadcasted_iota(jnp.int32, (COLS, CH), 0)
    for f, ref in enumerate(frames):
        for r in range(ROWS):
            slab = ref[r]
            wide = slab.astype(F32)
            left = jnp.where(row == 0, 0.0, pltpu.roll(wide, 1, axis=0))
            right = jnp.where(row == COLS - 1, 0.0, pltpu.roll(wide, COLS - 1, axis=0))
            spread[f, r, :, 0:CH] = left.astype(BF16)
            spread[f, r, :, CH : 2 * CH] = slab
            spread[f, r, :, 2 * CH : 3 * CH] = right.astype(BF16)


TAPS = [(1, 1), (0, 1), (2, 1), (0, 0), (1, 0), (2, 0), (0, 2), (1, 2), (2, 2)]


def row_range(b):
    return (ROWS, 0, 0) if b == 1 else (ROWS - 1, 1 if b == 2 else 0, 1 if b == 0 else 0)


def apply_tap(spread, weight, a, b, f0, count):
    rows, src, _ = row_range(b)
    piece = spread[f0 : f0 + count, src : src + rows].reshape(count * rows * COLS, 3 * CH)
    term = jnp.dot(piece, weight[a, b], preferred_element_type=F32)
    return term.reshape(count, rows, COLS, CH)


def inner_kernel(first, second, weight, acc, spread):
    spread_columns((first, second), spread)
    acc[...] = apply_tap(spread, weight, 1, 1, 0, 2)
    for a, b in TAPS[1:]:
        rows, _, dst = row_range(b)
        if a == 1:
            acc[:, dst : dst + rows] += apply_tap(spread, weight, a, b, 0, 2)
        elif a == 0:
            acc[1:2, dst : dst + rows] += apply_tap(spread, weight, a, b, 0, 1)
        else:
            acc[0:1, dst : dst + rows] += apply_tap(spread, weight, a, b, 1, 1)


def outer_taps(prev, follow, weight, acc, total, spread):
    spread_columns((prev, follow), spread)
    for f, a in ((0, 0), (1, 2)):
        total[f : f + 1] = acc[f : f + 1] + apply_tap(spread, weight, a, 1, f, 1)
        for b in (0, 2):
            rows, _, dst = row_range(b)
            total[f : f + 1, dst : dst + rows] += apply_tap(spread, weight, a, b, f, 1)


def forward_kernel(prev, follow, acc, weight, bias, head, pre, g0, g1, spread):
    outer_taps(prev, follow, weight, acc, pre, spread)
    for f, out in ((0, g0), (1, g1)):
        for r in range(ROWS):
            value = pre[f, r] + bias[...]
            pre[f, r] = value
            sig = jax.nn.sigmoid(value)
            slope = sig * (1.0 + value * (1.0 - sig))
            out[r] = (head[...] * slope).astype(BF16)


def transpose_kernel(prev, follow, acc, weight, g0, g1, spread, total):
    outer_taps(prev, follow, weight, acc, total, spread)
    for f, out in ((0, g0), (1, g1)):
        out[...] = total[f].astype(BF16)


def conv_scratch():
    return dict(
        spread=pltpu.VMEM((2, ROWS, COLS, 3 * CH), BF16),
        acc=pltpu.VMEM((2, ROWS, COLS, CH), F32),
    )


def turn_kernel(weight, bias, head, out, same, bias_out, head_out):
    for d in range(3):
        tap = weight[0, 0, d]
        same[0, 0, d] = tap
        out[0, 0, 2 - d] = tap.T
    bias_out[...] = bias[...]
    head_out[...] = head[...]


def turn_weights(weight, bias, head):
    full = jax.ShapeDtypeStruct((3, 3, 3, CH, CH), BF16)
    row = jax.ShapeDtypeStruct((1, CH), F32)
    here = pl.BlockSpec((1, 1, 3, CH, CH), lambda n: (n // 3, n % 3, 0, 0, 0))
    line = pl.BlockSpec((1, CH), lambda n: (0, 0))
    return pl.pallas_call(
        turn_kernel,
        grid=(9,),
        out_shape=(full, full, row, row),
        in_specs=[here, line, line],
        out_specs=(
            pl.BlockSpec((1, 1, 3, CH, CH), lambda n: (2 - n // 3, 2 - n % 3, 0, 0, 0)),
            here,
            line,
            line,
        ),
        compiler_params=params(8 << 20),
        cost_estimate=cost(2e9, 11 << 20),
        name="turn_weights",
    )(weight, bias, head)


FRAME = jax.ShapeDtypeStruct((ROWS, COLS, CH), BF16)
CONV_FLOPS = 2 * 1024 * 27 * CH * CH


def inner(first, second, w9, name):
    return pl.pallas_call(
        inner_kernel,
        out_shape=jax.ShapeDtypeStruct((2, ROWS, COLS, CH), F32),
        in_specs=[VMEM] * 3,
        out_specs=VMEM,
        scratch_shapes=[conv_scratch()["spread"]],
        compiler_params=params(),
        cost_estimate=cost(CONV_FLOPS * 2 / 3, 6 << 20),
        name=name,
    )(first, second, w9)


def forward(prev, follow, acc, w9, bias, head):
    return pl.pallas_call(
        forward_kernel,
        out_shape=(jax.ShapeDtypeStruct((2, ROWS, COLS, CH), F32), FRAME, FRAME),
        in_specs=[VMEM] * 6,
        out_specs=(VMEM, VMEM, VMEM),
        scratch_shapes=[conv_scratch()["spread"]],
        compiler_params=params(),
        cost_estimate=cost(CONV_FLOPS / 3, 6 << 20),
        name="forward",
    )(prev, follow, acc, w9, bias, head)


def transposed(prev, follow, acc, w9):
    s = conv_scratch()
    return pl.pallas_call(
        transpose_kernel,
        out_shape=(FRAME, FRAME),
        in_specs=[VMEM] * 4,
        out_specs=(VMEM, VMEM),
        scratch_shapes=[s["spread"], s["acc"]],
        compiler_params=params(),
        cost_estimate=cost(CONV_FLOPS / 3, 5 << 20),
        name="transposed",
    )(prev, follow, acc, w9)


def part_transposed(frames, x, turned):
    chan = lax.broadcasted_iota(jnp.int32, (PART, CH), 1)
    want = lax.broadcasted_iota(jnp.int32, (PART, CH), 0) + x * PART
    pick = jnp.where(chan == want, 1.0, 0.0).astype(BF16)
    width = ROWS * COLS
    lane = lax.rem(lax.broadcasted_iota(jnp.int32, (PART, width), 1), COLS)
    for f, ref in enumerate(frames):
        flat = ref[...].reshape(width, CH)
        mid = lax.dot_general(pick, flat, (((1,), (1,)), ((), ())), preferred_element_type=F32)
        left = jnp.where(lane == 0, 0.0, pltpu.roll(mid, 1, axis=1))
        right = jnp.where(lane == COLS - 1, 0.0, pltpu.roll(mid, width - 1, axis=1))
        at = slice(f * width, (f + 1) * width)
        turned[0:PART, at] = left.astype(BF16)
        turned[PART : 2 * PART, at] = mid.astype(BF16)
        turned[2 * PART : 3 * PART, at] = right.astype(BF16)


def turn_clips_kernel(pos, c0, c1, c2, c3, turned):
    part_transposed((c0, c1, c2, c3), pos[0], turned)


def turn_clips(pos, clips):
    return pl.pallas_call(
        turn_clips_kernel,
        out_shape=jax.ShapeDtypeStruct((3 * PART, 4 * ROWS * COLS), BF16),
        in_specs=[SMEM] + [VMEM] * 4,
        out_specs=VMEM,
        compiler_params=params(),
        cost_estimate=cost(1e9, 2 << 20),
        name="turn_clips",
    )(pos, *clips)


def correlate(turned, grads, b):
    width = ROWS * COLS
    rows = ROWS if b == 1 else ROWS - 1
    src = 1 if b == 2 else 0
    dst = 1 if b == 0 else 0
    left = []
    for a in range(3):
        parts = []
        for f in range(2):
            at = (a + f) * width + src * COLS
            parts.append(turned[:, at : at + rows * COLS])
        left.append(jnp.concatenate(parts, axis=1))
    left = jnp.concatenate(left, axis=0)
    right = [g[dst : dst + rows].reshape(rows * COLS, CH) for g in grads]
    return jnp.dot(left, jnp.concatenate(right, axis=0), preferred_element_type=F32)


def backward_kernel(
    pos, i0, i1, i2, i3, inside, turn_c, s0, s1, pre, weight, head, sent, kept,
    spread, acc, turn_i, pgb, total,
):
    x = pos[0]
    core = pos[1]
    grads = (i0, i1, i2, i3)
    part_transposed(grads, x, turn_i)
    outer_taps(i0, i3, weight, inside, acc, spread)
    sum_bias = jnp.zeros((8, CH), F32)
    sum_head = jnp.zeros((8, CH), F32)
    for f in range(2):
        for r in range(ROWS):
            back = PENALTY * acc[f, r]
            value = pre[f, r]
            sig = jax.nn.sigmoid(value)
            slope = sig * (1.0 + value * (1.0 - sig))
            curve = sig * (1.0 - sig) * (2.0 + value * (1.0 - 2.0 * sig))
            grad = back * head[...] * curve
            pgb[f, r] = grad.astype(BF16)
            sum_bias = sum_bias + jnp.sum(grad.reshape(COLS // 8, 8, CH), axis=0)
            sum_head = sum_head + jnp.sum((back * slope).reshape(COLS // 8, 8, CH), axis=0)
    total_bias = jnp.sum(sum_bias, axis=0, keepdims=True)
    total_head = jnp.sum(sum_head, axis=0, keepdims=True)
    row = lax.broadcasted_iota(jnp.int32, (8, CH), 0)
    small_bias = jnp.where(row == 0, total_bias, 0.0)
    small_head = jnp.where(row == 0, total_head, 0.0)
    blocks = []
    for b in range(3):
        block = PENALTY * correlate(turn_i, (s0, s1), b) + correlate(turn_c, (pgb.at[0], pgb.at[1]), b)
        blocks.append(block)
    for b, block in enumerate(blocks):
        total[b * 9 * PART : (b + 1) * 9 * PART] = block

    def store(out, h):
        lanes = slice(h * 128, (h + 1) * 128)
        for k in range(27):
            a, b, d = k // 9, (k // 3) % 3, k % 3
            at = ((b * 3 + a) * 3 + d) * PART
            out[k * 8 : (k + 1) * 8] = total[at : at + PART, lanes].reshape(PART // 8, 8, 128)
        out[TILES] = small_bias[:, lanes]
        out[TILES + 1] = small_head[:, lanes]
        out[TILES + 2 :] = jnp.zeros((PIECE * PIECES - TILES - 2, 8, 128), F32)

    @pl.when(core == 0)
    def _():
        store(kept, 0)
        store(sent, 1)

    @pl.when(core == 1)
    def _():
        store(kept, 1)
        store(sent, 0)


def backward(pos, grads, inside, turn_c, score, pre, w9, head):
    s = conv_scratch()
    return pl.pallas_call(
        backward_kernel,
        out_shape=(jax.ShapeDtypeStruct((PIECE * PIECES, 8, 128), F32),) * 2,
        in_specs=[SMEM] + [VMEM] * 11,
        out_specs=(VMEM, VMEM),
        scratch_shapes=[
            s["spread"],
            s["acc"],
            pltpu.VMEM((3 * PART, 4 * ROWS * COLS), BF16),
            pltpu.VMEM((2, ROWS, COLS, CH), BF16),
            pltpu.VMEM((27 * PART, CH), F32),
        ],
        compiler_params=params(),
        cost_estimate=cost(CONV_FLOPS * 1.6, 10 << 20),
        name="backward",
    )(pos, *grads, inside, turn_c, *score, pre, w9, head)


def relative(distance):
    return jnp.where(distance == 0, 0, jnp.where(distance == 3, 1, distance + 1))


def encode(value):
    most = jnp.max(jnp.abs(value), axis=1, keepdims=True)
    wide = (most * 1.004).astype(BF16).astype(F32)
    inverse = jnp.where(wide > 1e-37, 1.0 / jnp.maximum(wide, 1e-37), 0.0)
    code = jnp.exp2(jnp.abs(value) * inverse * SPAN - SPAN / 2)
    code = jnp.where(value < 0, -code, code).reshape(PIECE * 8, 128)
    tail = jnp.concatenate([wide.reshape(PIECE, 128), jnp.zeros((1, 128), F32)], axis=0)
    return jnp.concatenate([code, tail], axis=0).astype(BF16)


def encode_terms_kernel(kept, received, out):
    def step(n, _):
        at = pl.ds(n * PIECE, PIECE)
        out[n] = encode(kept[at] + received[at])
        return 0

    lax.fori_loop(0, PIECES, step, 0, unroll=4)


def encode_terms(kept, received):
    return pl.pallas_call(
        encode_terms_kernel,
        out_shape=jax.ShapeDtypeStruct((PIECES, CODED, 128), BF16),
        in_specs=[VMEM, VMEM],
        out_specs=VMEM,
        compiler_params=params(4 << 20),
        cost_estimate=cost(1e6, 3 << 20),
        name="encode_terms",
    )(kept, received)


def recode_kernel(pieces, out):
    def step(n, total):
        more = decode(pieces[n])
        return tuple(t + m for t, m in zip(total, more))

    zero = tuple(jnp.zeros((8, 128), F32) for _ in range(PIECE))
    total = lax.fori_loop(0, PIECES, step, zero, unroll=4)
    line = encode(jnp.stack(total))
    for n in range(8):
        out[n] = line


def recode(pieces):
    return pl.pallas_call(
        recode_kernel,
        out_shape=jax.ShapeDtypeStruct((8, CODED, 128), BF16),
        in_specs=[VMEM],
        out_specs=VMEM,
        compiler_params=params(4 << 20),
        cost_estimate=cost(1e6, 1 << 19),
        name="recode",
    )(pieces)


def decode(line):
    wide = line.astype(F32)
    level = jnp.log2(jnp.abs(wide[: PIECE * 8])) * (1.0 / SPAN) + 0.5
    level = jnp.where(wide[: PIECE * 8] < 0, -level, level)
    return [
        level[8 * j : 8 * j + 8] * wide[PIECE * 8 + j : PIECE * 8 + j + 1] for j in range(PIECE)
    ]


def assemble_kernel(pos, mine, other, out, small):
    x, core, y = pos[0], pos[1], pos[2]
    part = pl.program_id(0)
    at_x = relative(lax.rem(part - x + 4, 4))
    for ref, held in ((mine, core), (other, 1 - core)):
        lane = pl.ds(pl.multiple_of(held * 128, 128), 128)
        for row in range(4):
            at_y = relative(lax.rem(row - y + 4, 4))
            place = jnp.where(held == 0, at_x * 4 + at_y, at_y * 4 + at_x)
            for z in range(8):
                piece = ((row // 2) * 8 + z) * 2 + row % 2
                for j, value in enumerate(decode(ref[place, z])):
                    tile = piece * PIECE + j
                    if tile < TILES:
                        out[tile // 8, 0, tile % 8, :, lane] = value
                    elif tile < TILES + 2:
                        at = (tile - TILES) * 8
                        small[at : at + 8, lane] = value


def assemble(pos, mine, other):
    return pl.pallas_call(
        assemble_kernel,
        grid=(ROWS,),
        out_shape=(
            jax.ShapeDtypeStruct((27, ROWS, 8, 8, CH), F32),
            jax.ShapeDtypeStruct((16, CH), F32),
        ),
        in_specs=[SMEM, VMEM, VMEM],
        out_specs=(
            pl.BlockSpec((27, 1, 8, 8, CH), lambda i: (0, i, 0, 0, 0)),
            pl.BlockSpec((16, CH), lambda i: (0, 0)),
        ),
        compiler_params=params(),
        cost_estimate=cost(1e6, 15 << 20),
        name="assemble",
    )(pos, mine, other)


def ring_gather(value, plan):
    below = permute(value, plan(1))
    above = permute(value, plan(-1))
    half = value.shape[0] // 2
    across_low = permute(below[:half], plan(1))
    across_high = permute(above[half:], plan(-1))
    across = jnp.concatenate([across_low, across_high], axis=0)
    return jnp.stack([value, below, above, across])


def per_device(clips, weight, bias, head):
    x = lax.axis_index("x")
    core = lax.axis_index("c")
    y = lax.axis_index("yh") * 2 + lax.axis_index("yl")
    pos = jnp.stack([x, core, y]).astype(jnp.int32)
    own = clips.reshape(2, COLS, CH)
    below = permute(own, along_x(1))
    above = permute(own, along_x(-1))
    across = permute(own, along_x(2))
    turned, weight, bias, head = turn_weights(weight, bias.reshape(1, CH), head.reshape(1, CH))
    turned = turned.reshape(3, 3, 3 * CH, CH)
    w9 = weight.reshape(3, 3, 3 * CH, CH)

    c1, c2 = gather_rows(pos, own, below, above, across, bias)
    c0, c3 = chain(c2, 1), chain(c1, -1)
    pre, s0, s1 = forward(c0, c3, inner(c1, c2, w9, "forward_inner"), w9, bias, head)
    before, after = chain(s1, 1), chain(s0, -1)
    i1, i2 = transposed(before, after, inner(s0, s1, turned, "transposed_inner"), turned)
    turn_c = turn_clips(pos, (c0, c1, c2, c3))
    i0, i3 = chain(i2, 1), chain(i1, -1)
    inside = inner(i1, i2, w9, "backward_inner")
    sent, kept = backward(pos, (i0, i1, i2, i3), inside, turn_c, (s0, s1), pre, w9, head)
    coded = encode_terms(kept, permute(sent, swap_core))
    pieces = lax.all_to_all(coded, PLANE, 0, 0, tiled=True)
    line = lax.all_to_all(recode(pieces), "z", 0, 0, tiled=True)
    block = ring_gather(line, split_first)
    mine = ring_gather(block.reshape(32, CODED, 128), split_second)
    mine = mine.reshape(16, 8, CODED, 128)
    other = permute(mine, swap_core)
    grad_weight, small = assemble(pos, mine, other)
    return grad_weight.reshape(3, 3, 3, CH, CH), small[0], small[8]


def solution(mesh):
    fine = Mesh(mesh.devices.reshape(2, 8, 2, 2, 4), ALL)
    return jax.shard_map(
        per_device,
        mesh=fine,
        in_specs=(P("yh", CHAIN, "x", None, None), P(), P(), P()),
        out_specs=(P(), P(), P()),
        check_vma=False,
    )
```

```python
import functools

import jax
import jax.numpy as jnp
from jax import lax
from jax.experimental import pallas as pl
from jax.experimental.pallas import tpu as pltpu
from jax.sharding import Mesh, PartitionSpec as P

PENALTY = 0.01
F32 = jnp.float32
BF16 = jnp.bfloat16
ROWS = 4
COLS = 128
CH = 256
PART = CH // ROWS
TILES = 27 * PART // 8
PIECE = 7
PIECES = 32
CODED = 64
SPAN = 250.0
ALL = ("yh", "z", "yl", "c", "x")
PLANE = ("yh", "z", "yl")
CHAIN = ("z", "yl", "c")


def moved(fn):
    pairs = []
    for yh in range(2):
        for z in range(8):
            for yl in range(2):
                for c in range(2):
                    for x in range(4):
                        y2, z2, c2, x2 = fn(yh * 2 + yl, z, c, x)
                        y2, z2, x2 = y2 % 4, z2 % 8, x2 % 4
                        src = (((yh * 8 + z) * 2 + yl) * 2 + c) * 4 + x
                        dst = ((((y2 // 2) * 8 + z2) * 2 + y2 % 2) * 2 + c2) * 4 + x2
                        pairs.append((src, dst))
    return pairs


def permute(value, fn):
    return lax.ppermute(value, ALL, moved(fn))


def along_x(step):
    return lambda y, z, c, x: (y, z, c, x + step)


def swap_core(y, z, c, x):
    return (y, z, 1 - c, x)


def split_first(step):
    return lambda y, z, c, x: (y, z, c, x + step) if c else (y + step, z, c, x)


def split_second(step):
    return lambda y, z, c, x: (y + step, z, c, x) if c else (y, z, c, x + step)


def trade_far(value):
    pairs = []
    for i in range(1, 31, 2):
        pairs += [(i, i + 1), (i + 1, i)]
    return lax.ppermute(value, CHAIN, pairs)


def trade(near, far):
    return permute(near, swap_core), trade_far(far)


VMEM = pl.BlockSpec(memory_space=pltpu.VMEM)
SMEM = pl.BlockSpec(memory_space=pltpu.SMEM)


def params(limit=24 << 20):
    return pltpu.CompilerParams(vmem_limit_bytes=limit)


def cost(flops, nbytes):
    return pl.CostEstimate(flops=int(flops), bytes_accessed=int(nbytes), transcendentals=0)


def place_edges(core, first, second, near, far):
    @pl.when(core == 0)
    def _():
        near[...] = second[...]
        far[...] = first[...]

    @pl.when(core == 1)
    def _():
        near[...] = first[...]
        far[...] = second[...]


def gather_rows_kernel(pos_ref, own, below, above, across, ready, first, second, near, far):
    del ready
    x = pos_ref[0]
    for shift, ref in ((0, own), (3, below), (1, above), (2, across)):
        row = lax.rem(x + shift, 4)
        first[row] = ref[0]
        second[row] = ref[1]
    place_edges(pos_ref[1], first, second, near, far)


def gather_rows(pos, own, below, above, across, ready):
    out = jax.ShapeDtypeStruct((ROWS, COLS, CH), BF16)
    return pl.pallas_call(
        gather_rows_kernel,
        out_shape=(out,) * 4,
        in_specs=[SMEM] + [VMEM] * 5,
        out_specs=(VMEM,) * 4,
        compiler_params=params(),
        cost_estimate=cost(1e6, 1 << 20),
        name="gather_rows",
    )(pos, own, below, above, across, ready)


def spread_columns(frames, spread):
    row = lax.broadcasted_iota(jnp.int32, (COLS, CH), 0)
    for f, ref in enumerate(frames):
        for r in range(ROWS):
            slab = ref[r]
            wide = slab.astype(F32)
            left = jnp.where(row == 0, 0.0, pltpu.roll(wide, 1, axis=0))
            right = jnp.where(row == COLS - 1, 0.0, pltpu.roll(wide, COLS - 1, axis=0))
            spread[f, r, :, 0:CH] = left.astype(BF16)
            spread[f, r, :, CH : 2 * CH] = slab
            spread[f, r, :, 2 * CH : 3 * CH] = right.astype(BF16)


TAPS = [(1, 1), (0, 1), (2, 1), (0, 0), (1, 0), (2, 0), (0, 2), (1, 2), (2, 2)]


def row_range(b):
    return (ROWS, 0, 0) if b == 1 else (ROWS - 1, 1 if b == 2 else 0, 1 if b == 0 else 0)


def apply_tap(spread, weight, a, b, f0, count):
    rows, src, _ = row_range(b)
    piece = spread[f0 : f0 + count, src : src + rows].reshape(count * rows * COLS, 3 * CH)
    term = jnp.dot(piece, weight[a, b], preferred_element_type=F32)
    return term.reshape(count, rows, COLS, CH)


def inner_kernel(first, second, weight, acc, spread):
    spread_columns((first, second), spread)
    acc[...] = apply_tap(spread, weight, 1, 1, 0, 2)
    for a, b in TAPS[1:]:
        rows, _, dst = row_range(b)
        if a == 1:
            acc[:, dst : dst + rows] += apply_tap(spread, weight, a, b, 0, 2)
        elif a == 0:
            acc[1:2, dst : dst + rows] += apply_tap(spread, weight, a, b, 0, 1)
        else:
            acc[0:1, dst : dst + rows] += apply_tap(spread, weight, a, b, 1, 1)


def outer_taps(core, near, far, weight, acc, total, spread):
    spread_columns((near, far), spread)
    total[...] = acc[...]
    for n, f in ((0, 1 - core), (1, core)):
        at = pl.ds(f, 1)
        for b in (1, 0, 2):
            rows, _, dst = row_range(b)
            total[at, dst : dst + rows] += apply_tap(spread, weight, 2 * f, b, n, 1)


def forward_kernel(pos, near, far, acc, weight, bias, head, pre, g0, g1, near_out, far_out, spread):
    outer_taps(pos[1], near, far, weight, acc, pre, spread)
    for f, out in ((0, g0), (1, g1)):
        for r in range(ROWS):
            value = pre[f, r] + bias[...]
            pre[f, r] = value
            sig = jax.nn.sigmoid(value)
            slope = sig * (1.0 + value * (1.0 - sig))
            out[r] = (head[...] * slope).astype(BF16)
    place_edges(pos[1], g0, g1, near_out, far_out)


def transpose_kernel(pos, near, far, acc, weight, g0, g1, near_out, far_out, spread, total):
    outer_taps(pos[1], near, far, weight, acc, total, spread)
    for f, out in ((0, g0), (1, g1)):
        out[...] = total[f].astype(BF16)
    place_edges(pos[1], g0, g1, near_out, far_out)


def conv_scratch():
    return dict(
        spread=pltpu.VMEM((2, ROWS, COLS, 3 * CH), BF16),
        acc=pltpu.VMEM((2, ROWS, COLS, CH), F32),
    )


def turn_kernel(weight, bias, head, out, same, bias_out, head_out):
    for d in range(3):
        tap = weight[0, 0, d]
        same[0, 0, d] = tap
        out[0, 0, 2 - d] = tap.T
    bias_out[...] = bias[...]
    head_out[...] = head[...]


def turn_weights(weight, bias, head):
    full = jax.ShapeDtypeStruct((3, 3, 3, CH, CH), BF16)
    row = jax.ShapeDtypeStruct((1, CH), F32)
    here = pl.BlockSpec((1, 1, 3, CH, CH), lambda n: (n // 3, n % 3, 0, 0, 0))
    line = pl.BlockSpec((1, CH), lambda n: (0, 0))
    return pl.pallas_call(
        turn_kernel,
        grid=(9,),
        out_shape=(full, full, row, row),
        in_specs=[here, line, line],
        out_specs=(
            pl.BlockSpec((1, 1, 3, CH, CH), lambda n: (2 - n // 3, 2 - n % 3, 0, 0, 0)),
            here,
            line,
            line,
        ),
        compiler_params=params(8 << 20),
        cost_estimate=cost(2e9, 11 << 20),
        name="turn_weights",
    )(weight, bias, head)


FRAME = jax.ShapeDtypeStruct((ROWS, COLS, CH), BF16)
CONV_FLOPS = 2 * 1024 * 27 * CH * CH


def inner(first, second, w9, name):
    return pl.pallas_call(
        inner_kernel,
        out_shape=jax.ShapeDtypeStruct((2, ROWS, COLS, CH), F32),
        in_specs=[VMEM] * 3,
        out_specs=VMEM,
        scratch_shapes=[conv_scratch()["spread"]],
        compiler_params=params(),
        cost_estimate=cost(CONV_FLOPS * 2 / 3, 6 << 20),
        name=name,
    )(first, second, w9)


def forward(pos, near, far, acc, w9, bias, head):
    return pl.pallas_call(
        forward_kernel,
        out_shape=(jax.ShapeDtypeStruct((2, ROWS, COLS, CH), F32),) + (FRAME,) * 4,
        in_specs=[SMEM] + [VMEM] * 6,
        out_specs=(VMEM,) * 5,
        scratch_shapes=[conv_scratch()["spread"]],
        compiler_params=params(),
        cost_estimate=cost(CONV_FLOPS / 3, 6 << 20),
        name="forward",
    )(pos, near, far, acc, w9, bias, head)


def transposed(pos, near, far, acc, w9):
    s = conv_scratch()
    return pl.pallas_call(
        transpose_kernel,
        out_shape=(FRAME,) * 4,
        in_specs=[SMEM] + [VMEM] * 4,
        out_specs=(VMEM,) * 4,
        scratch_shapes=[s["spread"], s["acc"]],
        compiler_params=params(),
        cost_estimate=cost(CONV_FLOPS / 3, 5 << 20),
        name="transposed",
    )(pos, near, far, acc, w9)


def part_transposed(frames, pos, turned):
    chan = lax.broadcasted_iota(jnp.int32, (PART, CH), 1)
    want = lax.broadcasted_iota(jnp.int32, (PART, CH), 0) + pos[0] * PART
    pick = jnp.where(chan == want, 1.0, 0.0).astype(BF16)
    width = ROWS * COLS
    lane = lax.rem(lax.broadcasted_iota(jnp.int32, (PART, width), 1), COLS)
    core = pos[1]
    for f, ref in zip((3 - 3 * core, 1, 2, 3 * core), frames):
        flat = ref[...].reshape(width, CH)
        mid = lax.dot_general(pick, flat, (((1,), (1,)), ((), ())), preferred_element_type=F32)
        left = jnp.where(lane == 0, 0.0, pltpu.roll(mid, 1, axis=1))
        right = jnp.where(lane == COLS - 1, 0.0, pltpu.roll(mid, width - 1, axis=1))
        at = pl.ds(pl.multiple_of(f * width, width), width)
        turned[0:PART, at] = left.astype(BF16)
        turned[PART : 2 * PART, at] = mid.astype(BF16)
        turned[2 * PART : 3 * PART, at] = right.astype(BF16)


def turn_clips_kernel(pos, c0, c1, c2, c3, turned):
    part_transposed((c0, c1, c2, c3), pos, turned)


def turn_clips(pos, clips):
    return pl.pallas_call(
        turn_clips_kernel,
        out_shape=jax.ShapeDtypeStruct((3 * PART, 4 * ROWS * COLS), BF16),
        in_specs=[SMEM] + [VMEM] * 4,
        out_specs=VMEM,
        compiler_params=params(),
        cost_estimate=cost(1e9, 2 << 20),
        name="turn_clips",
    )(pos, *clips)


def correlate(turned, grads, b):
    width = ROWS * COLS
    rows = ROWS if b == 1 else ROWS - 1
    src = 1 if b == 2 else 0
    dst = 1 if b == 0 else 0
    left = []
    for a in range(3):
        parts = []
        for f in range(2):
            at = (a + f) * width + src * COLS
            parts.append(turned[:, at : at + rows * COLS])
        left.append(jnp.concatenate(parts, axis=1))
    left = jnp.concatenate(left, axis=0)
    right = [g[dst : dst + rows].reshape(rows * COLS, CH) for g in grads]
    return jnp.dot(left, jnp.concatenate(right, axis=0), preferred_element_type=F32)


def backward_kernel(
    pos, i0, i1, i2, i3, inside, turn_c, s0, s1, pre, weight, head, sent, kept,
    spread, acc, turn_i, pgb, total,
):
    core = pos[1]
    grads = (i0, i1, i2, i3)
    part_transposed(grads, pos, turn_i)
    outer_taps(core, i0, i3, weight, inside, acc, spread)
    sum_bias = jnp.zeros((8, CH), F32)
    sum_head = jnp.zeros((8, CH), F32)
    for f in range(2):
        for r in range(ROWS):
            back = PENALTY * acc[f, r]
            value = pre[f, r]
            sig = jax.nn.sigmoid(value)
            slope = sig * (1.0 + value * (1.0 - sig))
            curve = sig * (1.0 - sig) * (2.0 + value * (1.0 - 2.0 * sig))
            grad = back * head[...] * curve
            pgb[f, r] = grad.astype(BF16)
            sum_bias = sum_bias + jnp.sum(grad.reshape(COLS // 8, 8, CH), axis=0)
            sum_head = sum_head + jnp.sum((back * slope).reshape(COLS // 8, 8, CH), axis=0)
    total_bias = jnp.sum(sum_bias, axis=0, keepdims=True)
    total_head = jnp.sum(sum_head, axis=0, keepdims=True)
    row = lax.broadcasted_iota(jnp.int32, (8, CH), 0)
    small_bias = jnp.where(row == 0, total_bias, 0.0)
    small_head = jnp.where(row == 0, total_head, 0.0)
    blocks = []
    for b in range(3):
        block = PENALTY * correlate(turn_i, (s0, s1), b) + correlate(turn_c, (pgb.at[0], pgb.at[1]), b)
        blocks.append(block)
    for b, block in enumerate(blocks):
        total[b * 9 * PART : (b + 1) * 9 * PART] = block

    def store(out, h):
        lanes = slice(h * 128, (h + 1) * 128)
        for k in range(27):
            a, b, d = k // 9, (k // 3) % 3, k % 3
            at = ((b * 3 + a) * 3 + d) * PART
            out[k * 8 : (k + 1) * 8] = total[at : at + PART, lanes].reshape(PART // 8, 8, 128)
        out[TILES] = small_bias[:, lanes]
        out[TILES + 1] = small_head[:, lanes]
        out[TILES + 2 :] = jnp.zeros((PIECE * PIECES - TILES - 2, 8, 128), F32)

    @pl.when(core == 0)
    def _():
        store(kept, 0)
        store(sent, 1)

    @pl.when(core == 1)
    def _():
        store(kept, 1)
        store(sent, 0)


def backward(pos, grads, inside, turn_c, score, pre, w9, head):
    s = conv_scratch()
    return pl.pallas_call(
        backward_kernel,
        out_shape=(jax.ShapeDtypeStruct((PIECE * PIECES, 8, 128), F32),) * 2,
        in_specs=[SMEM] + [VMEM] * 11,
        out_specs=(VMEM, VMEM),
        scratch_shapes=[
            s["spread"],
            s["acc"],
            pltpu.VMEM((3 * PART, 4 * ROWS * COLS), BF16),
            pltpu.VMEM((2, ROWS, COLS, CH), BF16),
            pltpu.VMEM((27 * PART, CH), F32),
        ],
        compiler_params=params(),
        cost_estimate=cost(CONV_FLOPS * 1.6, 10 << 20),
        name="backward",
    )(pos, *grads, inside, turn_c, *score, pre, w9, head)


def relative(distance):
    return jnp.where(distance == 0, 0, jnp.where(distance == 3, 1, distance + 1))


def encode(value):
    most = jnp.max(jnp.abs(value), axis=1, keepdims=True)
    wide = (most * 1.004).astype(BF16).astype(F32)
    inverse = jnp.where(wide > 1e-37, 1.0 / jnp.maximum(wide, 1e-37), 0.0)
    code = jnp.exp2(jnp.abs(value) * inverse * SPAN - SPAN / 2)
    code = jnp.where(value < 0, -code, code).reshape(PIECE * 8, 128)
    tail = jnp.concatenate([wide.reshape(PIECE, 128), jnp.zeros((1, 128), F32)], axis=0)
    return jnp.concatenate([code, tail], axis=0).astype(BF16)


def encode_terms_kernel(kept, received, out):
    def step(n, _):
        at = pl.ds(n * PIECE, PIECE)
        out[n] = encode(kept[at] + received[at])
        return 0

    lax.fori_loop(0, PIECES, step, 0, unroll=4)


def encode_terms(kept, received):
    return pl.pallas_call(
        encode_terms_kernel,
        out_shape=jax.ShapeDtypeStruct((PIECES, CODED, 128), BF16),
        in_specs=[VMEM, VMEM],
        out_specs=VMEM,
        compiler_params=params(4 << 20),
        cost_estimate=cost(1e6, 3 << 20),
        name="encode_terms",
    )(kept, received)


def recode_kernel(pieces, out):
    def step(n, total):
        more = decode(pieces[n])
        return tuple(t + m for t, m in zip(total, more))

    zero = tuple(jnp.zeros((8, 128), F32) for _ in range(PIECE))
    total = lax.fori_loop(0, PIECES, step, zero, unroll=4)
    line = encode(jnp.stack(total))
    for n in range(8):
        out[n] = line


def recode(pieces):
    return pl.pallas_call(
        recode_kernel,
        out_shape=jax.ShapeDtypeStruct((8, CODED, 128), BF16),
        in_specs=[VMEM],
        out_specs=VMEM,
        compiler_params=params(4 << 20),
        cost_estimate=cost(1e6, 1 << 19),
        name="recode",
    )(pieces)


def decode(line):
    wide = line.astype(F32)
    level = jnp.log2(jnp.abs(wide[: PIECE * 8])) * (1.0 / SPAN) + 0.5
    level = jnp.where(wide[: PIECE * 8] < 0, -level, level)
    return [
        level[8 * j : 8 * j + 8] * wide[PIECE * 8 + j : PIECE * 8 + j + 1] for j in range(PIECE)
    ]


def assemble_kernel(pos, mine, other, out, small):
    x, core, y = pos[0], pos[1], pos[2]
    part = pl.program_id(0)
    at_x = relative(lax.rem(part - x + 4, 4))
    for ref, held in ((mine, core), (other, 1 - core)):
        lane = pl.ds(pl.multiple_of(held * 128, 128), 128)
        for row in range(4):
            at_y = relative(lax.rem(row - y + 4, 4))
            place = jnp.where(held == 0, at_x * 4 + at_y, at_y * 4 + at_x)
            for z in range(8):
                piece = ((row // 2) * 8 + z) * 2 + row % 2
                for j, value in enumerate(decode(ref[place, z])):
                    tile = piece * PIECE + j
                    if tile < TILES:
                        out[tile // 8, 0, tile % 8, :, lane] = value
                    elif tile < TILES + 2:
                        at = (tile - TILES) * 8
                        small[at : at + 8, lane] = value


def assemble(pos, mine, other):
    return pl.pallas_call(
        assemble_kernel,
        grid=(ROWS,),
        out_shape=(
            jax.ShapeDtypeStruct((27, ROWS, 8, 8, CH), F32),
            jax.ShapeDtypeStruct((16, CH), F32),
        ),
        in_specs=[SMEM, VMEM, VMEM],
        out_specs=(
            pl.BlockSpec((27, 1, 8, 8, CH), lambda i: (0, i, 0, 0, 0)),
            pl.BlockSpec((16, CH), lambda i: (0, 0)),
        ),
        compiler_params=params(),
        cost_estimate=cost(1e6, 15 << 20),
        name="assemble",
    )(pos, mine, other)


def ring_gather(value, plan, direct=False):
    below = permute(value, plan(1))
    above = permute(value, plan(-1))
    if direct:
        return jnp.stack([value, below, above, permute(value, plan(2))])
    half = value.shape[0] // 2
    across_low = permute(below[:half], plan(1))
    across_high = permute(above[half:], plan(-1))
    across = jnp.concatenate([across_low, across_high], axis=0)
    return jnp.stack([value, below, above, across])


def per_device(clips, weight, bias, head):
    x = lax.axis_index("x")
    core = lax.axis_index("c")
    y = lax.axis_index("yh") * 2 + lax.axis_index("yl")
    pos = jnp.stack([x, core, y]).astype(jnp.int32)
    own = clips.reshape(2, COLS, CH)
    below = permute(own, along_x(1))
    above = permute(own, along_x(-1))
    across = permute(own, along_x(2))
    turned, weight, bias, head = turn_weights(weight, bias.reshape(1, CH), head.reshape(1, CH))
    turned = turned.reshape(3, 3, 3 * CH, CH)
    w9 = weight.reshape(3, 3, 3 * CH, CH)

    c1, c2, near, far = gather_rows(pos, own, below, above, across, bias)
    c0, c3 = trade(near, far)
    acc = inner(c1, c2, w9, "forward_inner")
    pre, s0, s1, near, far = forward(pos, c0, c3, acc, w9, bias, head)
    near, far = trade(near, far)
    acc = inner(s0, s1, turned, "transposed_inner")
    i1, i2, edge, rim = transposed(pos, near, far, acc, turned)
    turn_c = turn_clips(pos, (c0, c1, c2, c3))
    i0, i3 = trade(edge, rim)
    inside = inner(i1, i2, w9, "backward_inner")
    sent, kept = backward(pos, (i0, i1, i2, i3), inside, turn_c, (s0, s1), pre, w9, head)
    coded = encode_terms(kept, permute(sent, swap_core))
    pieces = lax.all_to_all(coded, PLANE, 0, 0, tiled=True)
    line = lax.all_to_all(recode(pieces), "z", 0, 0, tiled=True)
    block = ring_gather(line, split_first, direct=True)
    mine = ring_gather(block.reshape(32, CODED, 128), split_second)
    mine = mine.reshape(16, 8, CODED, 128)
    other = permute(mine, swap_core)
    grad_weight, small = assemble(pos, mine, other)
    return grad_weight.reshape(3, 3, 3, CH, CH), small[0], small[8]


def solution(mesh):
    fine = Mesh(mesh.devices.reshape(2, 8, 2, 2, 4), ALL)
    return jax.shard_map(
        per_device,
        mesh=fine,
        in_specs=(P("yh", CHAIN, "x", None, None), P(), P(), P()),
        out_specs=(P(), P(), P()),
        check_vma=False,
    )
```

```python
import functools

import jax
import jax.numpy as jnp
from jax import lax
from jax.experimental import pallas as pl
from jax.experimental.pallas import tpu as pltpu
from jax.sharding import Mesh, PartitionSpec as P

PENALTY = 0.01
F32 = jnp.float32
BF16 = jnp.bfloat16
ROWS = 4
COLS = 128
CH = 256
PART = CH // ROWS
TILES = 27 * PART // 8
PIECE = 7
PIECES = 32
CODED = 64
SPAN = 250.0
ALL = ("yh", "z", "yl", "c", "x")
PLANE = ("yh", "z", "yl")
CHAIN = ("z", "yl", "c")


def moved(fn):
    pairs = []
    for yh in range(2):
        for z in range(8):
            for yl in range(2):
                for c in range(2):
                    for x in range(4):
                        y2, z2, c2, x2 = fn(yh * 2 + yl, z, c, x)
                        y2, z2, x2 = y2 % 4, z2 % 8, x2 % 4
                        src = (((yh * 8 + z) * 2 + yl) * 2 + c) * 4 + x
                        dst = ((((y2 // 2) * 8 + z2) * 2 + y2 % 2) * 2 + c2) * 4 + x2
                        pairs.append((src, dst))
    return pairs


def permute(value, fn):
    return lax.ppermute(value, ALL, moved(fn))


def along_x(step):
    return lambda y, z, c, x: (y, z, c, x + step)


def swap_core(y, z, c, x):
    return (y, z, 1 - c, x)


def split_first(step):
    return lambda y, z, c, x: (y, z, c, x + step) if c else (y + step, z, c, x)


def split_second(step):
    return lambda y, z, c, x: (y + step, z, c, x) if c else (y, z, c, x + step)


def trade_far(value):
    pairs = []
    for i in range(1, 31, 2):
        pairs += [(i, i + 1), (i + 1, i)]
    return lax.ppermute(value, CHAIN, pairs)


def trade(near, far):
    return permute(near, swap_core), trade_far(far)


VMEM = pl.BlockSpec(memory_space=pltpu.VMEM)
SMEM = pl.BlockSpec(memory_space=pltpu.SMEM)


def params(limit=24 << 20):
    return pltpu.CompilerParams(vmem_limit_bytes=limit)


def cost(flops, nbytes):
    return pl.CostEstimate(flops=int(flops), bytes_accessed=int(nbytes), transcendentals=0)


def place_edges(core, first, second, near, far):
    @pl.when(core == 0)
    def _():
        near[...] = second[...]
        far[...] = first[...]

    @pl.when(core == 1)
    def _():
        near[...] = first[...]
        far[...] = second[...]


def gather_rows_kernel(pos_ref, own, below, above, across, ready, first, second, near, far):
    del ready
    x = pos_ref[0]
    for shift, ref in ((0, own), (3, below), (1, above), (2, across)):
        row = lax.rem(x + shift, 4)
        first[row] = ref[0]
        second[row] = ref[1]
    place_edges(pos_ref[1], first, second, near, far)


def gather_rows(pos, own, below, above, across, ready):
    out = jax.ShapeDtypeStruct((ROWS, COLS, CH), BF16)
    return pl.pallas_call(
        gather_rows_kernel,
        out_shape=(out,) * 4,
        in_specs=[SMEM] + [VMEM] * 5,
        out_specs=(VMEM,) * 4,
        compiler_params=params(),
        cost_estimate=cost(1e6, 1 << 20),
        name="gather_rows",
    )(pos, own, below, above, across, ready)


def spread_columns(frames, spread):
    row = lax.broadcasted_iota(jnp.int32, (COLS, CH), 0)
    for f, ref in enumerate(frames):
        for r in range(ROWS):
            slab = ref[r]
            wide = slab.astype(F32)
            left = jnp.where(row == 0, 0.0, pltpu.roll(wide, 1, axis=0))
            right = jnp.where(row == COLS - 1, 0.0, pltpu.roll(wide, COLS - 1, axis=0))
            spread[f, r, :, 0:CH] = left.astype(BF16)
            spread[f, r, :, CH : 2 * CH] = slab
            spread[f, r, :, 2 * CH : 3 * CH] = right.astype(BF16)


TAPS = [(1, 1), (0, 1), (2, 1), (0, 0), (1, 0), (2, 0), (0, 2), (1, 2), (2, 2)]


def row_range(b):
    return (ROWS, 0, 0) if b == 1 else (ROWS - 1, 1 if b == 2 else 0, 1 if b == 0 else 0)


def apply_tap(spread, weight, a, b, f0, count):
    rows, src, _ = row_range(b)
    piece = spread[f0 : f0 + count, src : src + rows].reshape(count * rows * COLS, 3 * CH)
    term = jnp.dot(piece, weight[a, b], preferred_element_type=F32)
    return term.reshape(count, rows, COLS, CH)


def inner_kernel(first, second, weight, acc, spread):
    spread_columns((first, second), spread)
    acc[...] = apply_tap(spread, weight, 1, 1, 0, 2)
    for a, b in TAPS[1:]:
        rows, _, dst = row_range(b)
        if a == 1:
            acc[:, dst : dst + rows] += apply_tap(spread, weight, a, b, 0, 2)
        elif a == 0:
            acc[1:2, dst : dst + rows] += apply_tap(spread, weight, a, b, 0, 1)
        else:
            acc[0:1, dst : dst + rows] += apply_tap(spread, weight, a, b, 1, 1)


def side_taps(f, halo, weight, acc, total, spread):
    spread_columns((halo,), spread)
    at = pl.ds(f, 1)
    rest = pl.ds(1 - f, 1)
    total[rest] = acc[rest]
    total[at] = acc[at] + apply_tap(spread, weight, 2 * f, 1, 0, 1)
    for b in (0, 2):
        rows, _, dst = row_range(b)
        total[at, dst : dst + rows] += apply_tap(spread, weight, 2 * f, b, 0, 1)


def near_kernel(pos, near, acc, weight, total, spread):
    side_taps(1 - pos[1], near, weight, acc, total, spread)


def forward_kernel(pos, far, acc, weight, bias, head, pre, g0, g1, near_out, far_out, spread):
    side_taps(pos[1], far, weight, acc, pre, spread)
    for f, out in ((0, g0), (1, g1)):
        for r in range(ROWS):
            value = pre[f, r] + bias[...]
            pre[f, r] = value
            sig = jax.nn.sigmoid(value)
            slope = sig * (1.0 + value * (1.0 - sig))
            out[r] = (head[...] * slope).astype(BF16)
    place_edges(pos[1], g0, g1, near_out, far_out)


def transpose_kernel(pos, far, acc, weight, g0, g1, near_out, far_out, spread, total):
    side_taps(pos[1], far, weight, acc, total, spread)
    for f, out in ((0, g0), (1, g1)):
        out[...] = total[f].astype(BF16)
    place_edges(pos[1], g0, g1, near_out, far_out)


def conv_scratch():
    return dict(
        spread=pltpu.VMEM((2, ROWS, COLS, 3 * CH), BF16),
        acc=pltpu.VMEM((2, ROWS, COLS, CH), F32),
    )


def turn_kernel(weight, bias, head, out, same, bias_out, head_out):
    for d in range(3):
        tap = weight[0, 0, d]
        same[0, 0, d] = tap
        out[0, 0, 2 - d] = tap.T
    bias_out[...] = bias[...]
    head_out[...] = head[...]


def turn_weights(weight, bias, head):
    full = jax.ShapeDtypeStruct((3, 3, 3, CH, CH), BF16)
    row = jax.ShapeDtypeStruct((1, CH), F32)
    here = pl.BlockSpec((1, 1, 3, CH, CH), lambda n: (n // 3, n % 3, 0, 0, 0))
    line = pl.BlockSpec((1, CH), lambda n: (0, 0))
    return pl.pallas_call(
        turn_kernel,
        grid=(9,),
        out_shape=(full, full, row, row),
        in_specs=[here, line, line],
        out_specs=(
            pl.BlockSpec((1, 1, 3, CH, CH), lambda n: (2 - n // 3, 2 - n % 3, 0, 0, 0)),
            here,
            line,
            line,
        ),
        compiler_params=params(8 << 20),
        cost_estimate=cost(2e9, 11 << 20),
        name="turn_weights",
    )(weight, bias, head)


FRAME = jax.ShapeDtypeStruct((ROWS, COLS, CH), BF16)
CONV_FLOPS = 2 * 1024 * 27 * CH * CH


def inner(first, second, w9, name):
    return pl.pallas_call(
        inner_kernel,
        out_shape=jax.ShapeDtypeStruct((2, ROWS, COLS, CH), F32),
        in_specs=[VMEM] * 3,
        out_specs=VMEM,
        scratch_shapes=[conv_scratch()["spread"]],
        compiler_params=params(),
        cost_estimate=cost(CONV_FLOPS * 2 / 3, 6 << 20),
        name=name,
    )(first, second, w9)


def forward(pos, far, acc, w9, bias, head):
    return pl.pallas_call(
        forward_kernel,
        out_shape=(jax.ShapeDtypeStruct((2, ROWS, COLS, CH), F32),) + (FRAME,) * 4,
        in_specs=[SMEM] + [VMEM] * 5,
        out_specs=(VMEM,) * 5,
        scratch_shapes=[conv_scratch()["spread"]],
        compiler_params=params(),
        cost_estimate=cost(CONV_FLOPS / 3, 6 << 20),
        name="forward",
    )(pos, far, acc, w9, bias, head)


def add_near(pos, near, acc, w9, name):
    return pl.pallas_call(
        near_kernel,
        out_shape=jax.ShapeDtypeStruct((2, ROWS, COLS, CH), F32),
        in_specs=[SMEM] + [VMEM] * 3,
        out_specs=VMEM,
        scratch_shapes=[conv_scratch()["spread"]],
        compiler_params=params(),
        cost_estimate=cost(CONV_FLOPS / 6, 4 << 20),
        name=name,
    )(pos, near, acc, w9)


def transposed(pos, far, acc, w9):
    s = conv_scratch()
    return pl.pallas_call(
        transpose_kernel,
        out_shape=(FRAME,) * 4,
        in_specs=[SMEM] + [VMEM] * 3,
        out_specs=(VMEM,) * 4,
        scratch_shapes=[s["spread"], s["acc"]],
        compiler_params=params(),
        cost_estimate=cost(CONV_FLOPS / 3, 5 << 20),
        name="transposed",
    )(pos, far, acc, w9)


def part_transposed(frames, pos, turned):
    chan = lax.broadcasted_iota(jnp.int32, (PART, CH), 1)
    want = lax.broadcasted_iota(jnp.int32, (PART, CH), 0) + pos[0] * PART
    pick = jnp.where(chan == want, 1.0, 0.0).astype(BF16)
    width = ROWS * COLS
    lane = lax.rem(lax.broadcasted_iota(jnp.int32, (PART, width), 1), COLS)
    core = pos[1]
    for f, ref in zip((3 - 3 * core, 1, 2, 3 * core), frames):
        flat = ref[...].reshape(width, CH)
        mid = lax.dot_general(pick, flat, (((1,), (1,)), ((), ())), preferred_element_type=F32)
        left = jnp.where(lane == 0, 0.0, pltpu.roll(mid, 1, axis=1))
        right = jnp.where(lane == COLS - 1, 0.0, pltpu.roll(mid, width - 1, axis=1))
        at = pl.ds(pl.multiple_of(f * width, width), width)
        turned[0:PART, at] = left.astype(BF16)
        turned[PART : 2 * PART, at] = mid.astype(BF16)
        turned[2 * PART : 3 * PART, at] = right.astype(BF16)


def near_turn_kernel(pos, near, acc, weight, c0, c1, c2, c3, total, turned, spread):
    side_taps(1 - pos[1], near, weight, acc, total, spread)
    part_transposed((c0, c1, c2, c3), pos, turned)


def add_near_turn(pos, near, acc, w9, clips):
    return pl.pallas_call(
        near_turn_kernel,
        out_shape=(
            jax.ShapeDtypeStruct((2, ROWS, COLS, CH), F32),
            jax.ShapeDtypeStruct((3 * PART, 4 * ROWS * COLS), BF16),
        ),
        in_specs=[SMEM] + [VMEM] * 7,
        out_specs=(VMEM, VMEM),
        scratch_shapes=[conv_scratch()["spread"]],
        compiler_params=params(),
        cost_estimate=cost(CONV_FLOPS / 4, 6 << 20),
        name="transposed_near",
    )(pos, near, acc, w9, *clips)


def correlate(turned, grads, b):
    width = ROWS * COLS
    rows = ROWS if b == 1 else ROWS - 1
    src = 1 if b == 2 else 0
    dst = 1 if b == 0 else 0
    left = []
    for a in range(3):
        parts = []
        for f in range(2):
            at = (a + f) * width + src * COLS
            parts.append(turned[:, at : at + rows * COLS])
        left.append(jnp.concatenate(parts, axis=1))
    left = jnp.concatenate(left, axis=0)
    right = [g[dst : dst + rows].reshape(rows * COLS, CH) for g in grads]
    return jnp.dot(left, jnp.concatenate(right, axis=0), preferred_element_type=F32)


def backward_kernel(
    pos, i0, i1, i2, i3, inside, turn_c, s0, s1, pre, weight, head, sent, kept,
    spread, acc, turn_i, pgb, total,
):
    core = pos[1]
    grads = (i0, i1, i2, i3)
    part_transposed(grads, pos, turn_i)
    side_taps(core, i3, weight, inside, acc, spread)
    sum_bias = jnp.zeros((8, CH), F32)
    sum_head = jnp.zeros((8, CH), F32)
    for f in range(2):
        for r in range(ROWS):
            back = PENALTY * acc[f, r]
            value = pre[f, r]
            sig = jax.nn.sigmoid(value)
            slope = sig * (1.0 + value * (1.0 - sig))
            curve = sig * (1.0 - sig) * (2.0 + value * (1.0 - 2.0 * sig))
            grad = back * head[...] * curve
            pgb[f, r] = grad.astype(BF16)
            sum_bias = sum_bias + jnp.sum(grad.reshape(COLS // 8, 8, CH), axis=0)
            sum_head = sum_head + jnp.sum((back * slope).reshape(COLS // 8, 8, CH), axis=0)
    total_bias = jnp.sum(sum_bias, axis=0, keepdims=True)
    total_head = jnp.sum(sum_head, axis=0, keepdims=True)
    row = lax.broadcasted_iota(jnp.int32, (8, CH), 0)
    small_bias = jnp.where(row == 0, total_bias, 0.0)
    small_head = jnp.where(row == 0, total_head, 0.0)
    blocks = []
    for b in range(3):
        block = PENALTY * correlate(turn_i, (s0, s1), b) + correlate(turn_c, (pgb.at[0], pgb.at[1]), b)
        blocks.append(block)
    for b, block in enumerate(blocks):
        total[b * 9 * PART : (b + 1) * 9 * PART] = block

    def store(out, h):
        lanes = slice(h * 128, (h + 1) * 128)
        for k in range(27):
            a, b, d = k // 9, (k // 3) % 3, k % 3
            at = ((b * 3 + a) * 3 + d) * PART
            out[k * 8 : (k + 1) * 8] = total[at : at + PART, lanes].reshape(PART // 8, 8, 128)
        out[TILES] = small_bias[:, lanes]
        out[TILES + 1] = small_head[:, lanes]
        out[TILES + 2 :] = jnp.zeros((PIECE * PIECES - TILES - 2, 8, 128), F32)

    @pl.when(core == 0)
    def _():
        store(kept, 0)
        store(sent, 1)

    @pl.when(core == 1)
    def _():
        store(kept, 1)
        store(sent, 0)


def backward(pos, grads, inside, turn_c, score, pre, w9, head):
    s = conv_scratch()
    return pl.pallas_call(
        backward_kernel,
        out_shape=(jax.ShapeDtypeStruct((PIECE * PIECES, 8, 128), F32),) * 2,
        in_specs=[SMEM] + [VMEM] * 11,
        out_specs=(VMEM, VMEM),
        scratch_shapes=[
            s["spread"],
            s["acc"],
            pltpu.VMEM((3 * PART, 4 * ROWS * COLS), BF16),
            pltpu.VMEM((2, ROWS, COLS, CH), BF16),
            pltpu.VMEM((27 * PART, CH), F32),
        ],
        compiler_params=params(),
        cost_estimate=cost(CONV_FLOPS * 1.6, 10 << 20),
        name="backward",
    )(pos, *grads, inside, turn_c, *score, pre, w9, head)


def relative(distance):
    return jnp.where(distance == 0, 0, jnp.where(distance == 3, 1, distance + 1))


def encode(value):
    most = jnp.max(jnp.abs(value), axis=1, keepdims=True)
    wide = (most * 1.004).astype(BF16).astype(F32)
    inverse = jnp.where(wide > 1e-37, 1.0 / jnp.maximum(wide, 1e-37), 0.0)
    code = jnp.exp2(jnp.abs(value) * inverse * SPAN - SPAN / 2)
    code = jnp.where(value < 0, -code, code).reshape(PIECE * 8, 128)
    tail = jnp.concatenate([wide.reshape(PIECE, 128), jnp.zeros((1, 128), F32)], axis=0)
    return jnp.concatenate([code, tail], axis=0).astype(BF16)


def encode_terms_kernel(kept, received, out):
    def step(n, _):
        at = pl.ds(n * PIECE, PIECE)
        out[n] = encode(kept[at] + received[at])
        return 0

    lax.fori_loop(0, PIECES, step, 0, unroll=4)


def encode_terms(kept, received):
    return pl.pallas_call(
        encode_terms_kernel,
        out_shape=jax.ShapeDtypeStruct((PIECES, CODED, 128), BF16),
        in_specs=[VMEM, VMEM],
        out_specs=VMEM,
        compiler_params=params(4 << 20),
        cost_estimate=cost(1e6, 3 << 20),
        name="encode_terms",
    )(kept, received)


def recode_kernel(pieces, out):
    def step(n, total):
        more = decode(pieces[n])
        return tuple(t + m for t, m in zip(total, more))

    zero = tuple(jnp.zeros((8, 128), F32) for _ in range(PIECE))
    total = lax.fori_loop(0, PIECES, step, zero, unroll=4)
    line = encode(jnp.stack(total))
    for n in range(8):
        out[n] = line


def recode(pieces):
    return pl.pallas_call(
        recode_kernel,
        out_shape=jax.ShapeDtypeStruct((8, CODED, 128), BF16),
        in_specs=[VMEM],
        out_specs=VMEM,
        compiler_params=params(4 << 20),
        cost_estimate=cost(1e6, 1 << 19),
        name="recode",
    )(pieces)


def decode(line):
    wide = line.astype(F32)
    level = jnp.log2(jnp.abs(wide[: PIECE * 8])) * (1.0 / SPAN) + 0.5
    level = jnp.where(wide[: PIECE * 8] < 0, -level, level)
    return [
        level[8 * j : 8 * j + 8] * wide[PIECE * 8 + j : PIECE * 8 + j + 1] for j in range(PIECE)
    ]


def assemble_kernel(pos, mine, other, out, small):
    x, core, y = pos[0], pos[1], pos[2]
    part = pl.program_id(0)
    at_x = relative(lax.rem(part - x + 4, 4))
    for ref, held in ((mine, core), (other, 1 - core)):
        lane = pl.ds(pl.multiple_of(held * 128, 128), 128)
        for row in range(4):
            at_y = relative(lax.rem(row - y + 4, 4))
            place = jnp.where(held == 0, at_x * 4 + at_y, at_y * 4 + at_x)
            for z in range(8):
                piece = ((row // 2) * 8 + z) * 2 + row % 2
                for j, value in enumerate(decode(ref[place, z])):
                    tile = piece * PIECE + j
                    if tile < TILES:
                        out[tile // 8, 0, tile % 8, :, lane] = value
                    elif tile < TILES + 2:
                        at = (tile - TILES) * 8
                        small[at : at + 8, lane] = value


def assemble(pos, mine, other):
    return pl.pallas_call(
        assemble_kernel,
        grid=(ROWS,),
        out_shape=(
            jax.ShapeDtypeStruct((27, ROWS, 8, 8, CH), F32),
            jax.ShapeDtypeStruct((16, CH), F32),
        ),
        in_specs=[SMEM, VMEM, VMEM],
        out_specs=(
            pl.BlockSpec((27, 1, 8, 8, CH), lambda i: (0, i, 0, 0, 0)),
            pl.BlockSpec((16, CH), lambda i: (0, 0)),
        ),
        compiler_params=params(),
        cost_estimate=cost(1e6, 15 << 20),
        name="assemble",
    )(pos, mine, other)


def ring_gather(value, plan, direct=False):
    below = permute(value, plan(1))
    above = permute(value, plan(-1))
    if direct:
        return jnp.stack([value, below, above, permute(value, plan(2))])
    half = value.shape[0] // 2
    across_low = permute(below[:half], plan(1))
    across_high = permute(above[half:], plan(-1))
    across = jnp.concatenate([across_low, across_high], axis=0)
    return jnp.stack([value, below, above, across])


def per_device(clips, weight, bias, head):
    x = lax.axis_index("x")
    core = lax.axis_index("c")
    y = lax.axis_index("yh") * 2 + lax.axis_index("yl")
    pos = jnp.stack([x, core, y]).astype(jnp.int32)
    own = clips.reshape(2, COLS, CH)
    below = permute(own, along_x(1))
    above = permute(own, along_x(-1))
    across = permute(own, along_x(2))
    turned, weight, bias, head = turn_weights(weight, bias.reshape(1, CH), head.reshape(1, CH))
    turned = turned.reshape(3, 3, 3 * CH, CH)
    w9 = weight.reshape(3, 3, 3 * CH, CH)

    c1, c2, near, far = gather_rows(pos, own, below, above, across, bias)
    c0, c3 = trade(near, far)
    acc = add_near(pos, c0, inner(c1, c2, w9, "forward_inner"), w9, "forward_near")
    pre, s0, s1, near, far = forward(pos, c3, acc, w9, bias, head)
    near, far = trade(near, far)
    acc = inner(s0, s1, turned, "transposed_inner")
    acc, turn_c = add_near_turn(pos, near, acc, turned, (c0, c1, c2, c3))
    i1, i2, edge, rim = transposed(pos, far, acc, turned)
    i0, i3 = trade(edge, rim)
    inside = inner(i1, i2, w9, "backward_inner")
    inside = add_near(pos, i0, inside, w9, "backward_near")
    sent, kept = backward(pos, (i0, i1, i2, i3), inside, turn_c, (s0, s1), pre, w9, head)
    coded = encode_terms(kept, permute(sent, swap_core))
    pieces = lax.all_to_all(coded, PLANE, 0, 0, tiled=True)
    line = lax.all_to_all(recode(pieces), "z", 0, 0, tiled=True)
    block = ring_gather(line, split_first, direct=True)
    mine = ring_gather(block.reshape(32, CODED, 128), split_second)
    mine = mine.reshape(16, 8, CODED, 128)
    other = permute(mine, swap_core)
    grad_weight, small = assemble(pos, mine, other)
    return grad_weight.reshape(3, 3, 3, CH, CH), small[0], small[8]


def solution(mesh):
    fine = Mesh(mesh.devices.reshape(2, 8, 2, 2, 4), ALL)
    return jax.shard_map(
        per_device,
        mesh=fine,
        in_specs=(P("yh", CHAIN, "x", None, None), P(), P(), P()),
        out_specs=(P(), P(), P()),
        check_vma=False,
    )
```

```python
import functools

import jax
import jax.numpy as jnp
from jax import lax
from jax.experimental import pallas as pl
from jax.experimental.pallas import tpu as pltpu
from jax.sharding import Mesh, PartitionSpec as P

PENALTY = 0.01
F32 = jnp.float32
BF16 = jnp.bfloat16
ROWS = 4
COLS = 128
CH = 256
PART = CH // ROWS
TILES = 27 * PART // 8
PIECE = 7
PIECES = 32
CODED = 64
SPAN = 250.0
ALL = ("yh", "z", "yl", "c", "x")
PLANE = ("yh", "z", "yl")
CHAIN = ("z", "yl", "c")


def moved(fn):
    pairs = []
    for yh in range(2):
        for z in range(8):
            for yl in range(2):
                for c in range(2):
                    for x in range(4):
                        y2, z2, c2, x2 = fn(yh * 2 + yl, z, c, x)
                        y2, z2, x2 = y2 % 4, z2 % 8, x2 % 4
                        src = (((yh * 8 + z) * 2 + yl) * 2 + c) * 4 + x
                        dst = ((((y2 // 2) * 8 + z2) * 2 + y2 % 2) * 2 + c2) * 4 + x2
                        pairs.append((src, dst))
    return pairs


def permute(value, fn):
    return lax.ppermute(value, ALL, moved(fn))


def along_x(step):
    return lambda y, z, c, x: (y, z, c, x + step)


def swap_core(y, z, c, x):
    return (y, z, 1 - c, x)


def split_first(step):
    return lambda y, z, c, x: (y + step, z, c, x) if c else (y, z, c, x + step)


def split_second(step):
    return lambda y, z, c, x: (y, z, c, x + step) if c else (y + step, z, c, x)


def trade_far(value):
    pairs = []
    for i in range(1, 31, 2):
        pairs += [(i, i + 1), (i + 1, i)]
    return lax.ppermute(value, CHAIN, pairs)


def trade(near, far):
    return permute(near, swap_core), trade_far(far)


VMEM = pl.BlockSpec(memory_space=pltpu.VMEM)
SMEM = pl.BlockSpec(memory_space=pltpu.SMEM)


def params(limit=24 << 20):
    return pltpu.CompilerParams(vmem_limit_bytes=limit)


def cost(flops, nbytes):
    return pl.CostEstimate(flops=int(flops), bytes_accessed=int(nbytes), transcendentals=0)


def place_edges(core, first, second, near, far):
    @pl.when(core == 0)
    def _():
        near[...] = second[...]
        far[...] = first[...]

    @pl.when(core == 1)
    def _():
        near[...] = first[...]
        far[...] = second[...]


def gather_rows_kernel(pos_ref, own, below, above, across, ready, first, second, near, far):
    del ready
    x = pos_ref[0]
    for shift, ref in ((0, own), (3, below), (1, above), (2, across)):
        row = lax.rem(x + shift, 4)
        first[row] = ref[0]
        second[row] = ref[1]
    place_edges(pos_ref[1], first, second, near, far)


def gather_rows(pos, own, below, above, across, ready):
    out = jax.ShapeDtypeStruct((ROWS, COLS, CH), BF16)
    return pl.pallas_call(
        gather_rows_kernel,
        out_shape=(out,) * 4,
        in_specs=[SMEM] + [VMEM] * 5,
        out_specs=(VMEM,) * 4,
        compiler_params=params(),
        cost_estimate=cost(1e6, 1 << 20),
        name="gather_rows",
    )(pos, own, below, above, across, ready)


def spread_columns(frames, spread):
    row = lax.broadcasted_iota(jnp.int32, (COLS, CH), 0)
    for f, ref in enumerate(frames):
        for r in range(ROWS):
            slab = ref[r]
            wide = slab.astype(F32)
            left = jnp.where(row == 0, 0.0, pltpu.roll(wide, 1, axis=0))
            right = jnp.where(row == COLS - 1, 0.0, pltpu.roll(wide, COLS - 1, axis=0))
            spread[f, r, :, 0:CH] = left.astype(BF16)
            spread[f, r, :, CH : 2 * CH] = slab
            spread[f, r, :, 2 * CH : 3 * CH] = right.astype(BF16)


TAPS = [(1, 1), (0, 1), (2, 1), (0, 0), (1, 0), (2, 0), (0, 2), (1, 2), (2, 2)]


def row_range(b):
    return (ROWS, 0, 0) if b == 1 else (ROWS - 1, 1 if b == 2 else 0, 1 if b == 0 else 0)


def apply_tap(spread, weight, a, b, f0, count):
    rows, src, _ = row_range(b)
    piece = spread[f0 : f0 + count, src : src + rows].reshape(count * rows * COLS, 3 * CH)
    term = jnp.dot(piece, weight[a, b], preferred_element_type=F32)
    return term.reshape(count, rows, COLS, CH)


def inner_kernel(first, second, weight, acc, spread):
    spread_columns((first, second), spread)
    acc[...] = apply_tap(spread, weight, 1, 1, 0, 2)
    for a, b in TAPS[1:]:
        rows, _, dst = row_range(b)
        if a == 1:
            acc[:, dst : dst + rows] += apply_tap(spread, weight, a, b, 0, 2)
        elif a == 0:
            acc[1:2, dst : dst + rows] += apply_tap(spread, weight, a, b, 0, 1)
        else:
            acc[0:1, dst : dst + rows] += apply_tap(spread, weight, a, b, 1, 1)


def side_taps(f, halo, weight, acc, total, spread):
    spread_columns((halo,), spread)
    at = pl.ds(f, 1)
    rest = pl.ds(1 - f, 1)
    total[rest] = acc[rest]
    total[at] = acc[at] + apply_tap(spread, weight, 2 * f, 1, 0, 1)
    for b in (0, 2):
        rows, _, dst = row_range(b)
        total[at, dst : dst + rows] += apply_tap(spread, weight, 2 * f, b, 0, 1)


def near_kernel(pos, near, acc, weight, total, spread):
    side_taps(1 - pos[1], near, weight, acc, total, spread)


def forward_kernel(pos, far, acc, weight, bias, head, pre, g0, g1, near_out, far_out, spread):
    side_taps(pos[1], far, weight, acc, pre, spread)
    for f, out in ((0, g0), (1, g1)):
        for r in range(ROWS):
            value = pre[f, r] + bias[...]
            pre[f, r] = value
            sig = jax.nn.sigmoid(value)
            slope = sig * (1.0 + value * (1.0 - sig))
            out[r] = (head[...] * slope).astype(BF16)
    place_edges(pos[1], g0, g1, near_out, far_out)


def transpose_kernel(pos, far, acc, weight, g0, g1, near_out, far_out, spread, total):
    side_taps(pos[1], far, weight, acc, total, spread)
    for f, out in ((0, g0), (1, g1)):
        out[...] = total[f].astype(BF16)
    place_edges(pos[1], g0, g1, near_out, far_out)


def conv_scratch():
    return dict(
        spread=pltpu.VMEM((2, ROWS, COLS, 3 * CH), BF16),
        acc=pltpu.VMEM((2, ROWS, COLS, CH), F32),
    )


def turn_kernel(weight, bias, head, out, same, bias_out, head_out):
    for d in range(3):
        tap = weight[0, 0, d]
        same[0, 0, d] = tap
        out[0, 0, 2 - d] = tap.T
    bias_out[...] = bias[...]
    head_out[...] = head[...]


def turn_weights(weight, bias, head):
    full = jax.ShapeDtypeStruct((3, 3, 3, CH, CH), BF16)
    row = jax.ShapeDtypeStruct((1, CH), F32)
    here = pl.BlockSpec((1, 1, 3, CH, CH), lambda n: (n // 3, n % 3, 0, 0, 0))
    line = pl.BlockSpec((1, CH), lambda n: (0, 0))
    return pl.pallas_call(
        turn_kernel,
        grid=(9,),
        out_shape=(full, full, row, row),
        in_specs=[here, line, line],
        out_specs=(
            pl.BlockSpec((1, 1, 3, CH, CH), lambda n: (2 - n // 3, 2 - n % 3, 0, 0, 0)),
            here,
            line,
            line,
        ),
        compiler_params=params(8 << 20),
        cost_estimate=cost(2e9, 11 << 20),
        name="turn_weights",
    )(weight, bias, head)


FRAME = jax.ShapeDtypeStruct((ROWS, COLS, CH), BF16)
CONV_FLOPS = 2 * 1024 * 27 * CH * CH


def inner(first, second, w9, name):
    return pl.pallas_call(
        inner_kernel,
        out_shape=jax.ShapeDtypeStruct((2, ROWS, COLS, CH), F32),
        in_specs=[VMEM] * 3,
        out_specs=VMEM,
        scratch_shapes=[conv_scratch()["spread"]],
        compiler_params=params(),
        cost_estimate=cost(CONV_FLOPS * 2 / 3, 6 << 20),
        name=name,
    )(first, second, w9)


def forward(pos, far, acc, w9, bias, head):
    return pl.pallas_call(
        forward_kernel,
        out_shape=(jax.ShapeDtypeStruct((2, ROWS, COLS, CH), F32),) + (FRAME,) * 4,
        in_specs=[SMEM] + [VMEM] * 5,
        out_specs=(VMEM,) * 5,
        scratch_shapes=[conv_scratch()["spread"]],
        compiler_params=params(),
        cost_estimate=cost(CONV_FLOPS / 3, 6 << 20),
        name="forward",
    )(pos, far, acc, w9, bias, head)


def add_near(pos, near, acc, w9, name):
    return pl.pallas_call(
        near_kernel,
        out_shape=jax.ShapeDtypeStruct((2, ROWS, COLS, CH), F32),
        in_specs=[SMEM] + [VMEM] * 3,
        out_specs=VMEM,
        scratch_shapes=[conv_scratch()["spread"]],
        compiler_params=params(),
        cost_estimate=cost(CONV_FLOPS / 6, 4 << 20),
        name=name,
    )(pos, near, acc, w9)


def transposed(pos, far, acc, w9):
    s = conv_scratch()
    return pl.pallas_call(
        transpose_kernel,
        out_shape=(FRAME,) * 4,
        in_specs=[SMEM] + [VMEM] * 3,
        out_specs=(VMEM,) * 4,
        scratch_shapes=[s["spread"], s["acc"]],
        compiler_params=params(),
        cost_estimate=cost(CONV_FLOPS / 3, 5 << 20),
        name="transposed",
    )(pos, far, acc, w9)


def part_transposed(frames, pos, turned):
    chan = lax.broadcasted_iota(jnp.int32, (PART, CH), 1)
    want = lax.broadcasted_iota(jnp.int32, (PART, CH), 0) + pos[0] * PART
    pick = jnp.where(chan == want, 1.0, 0.0).astype(BF16)
    width = ROWS * COLS
    lane = lax.rem(lax.broadcasted_iota(jnp.int32, (PART, width), 1), COLS)
    core = pos[1]
    for f, ref in zip((3 - 3 * core, 1, 2, 3 * core), frames):
        flat = ref[...].reshape(width, CH)
        mid = lax.dot_general(pick, flat, (((1,), (1,)), ((), ())), preferred_element_type=F32)
        left = jnp.where(lane == 0, 0.0, pltpu.roll(mid, 1, axis=1))
        right = jnp.where(lane == COLS - 1, 0.0, pltpu.roll(mid, width - 1, axis=1))
        at = pl.ds(pl.multiple_of(f * width, width), width)
        turned[0:PART, at] = left.astype(BF16)
        turned[PART : 2 * PART, at] = mid.astype(BF16)
        turned[2 * PART : 3 * PART, at] = right.astype(BF16)


def near_turn_kernel(pos, near, acc, weight, c0, c1, c2, c3, total, turned, spread):
    side_taps(1 - pos[1], near, weight, acc, total, spread)
    part_transposed((c0, c1, c2, c3), pos, turned)


def add_near_turn(pos, near, acc, w9, clips):
    return pl.pallas_call(
        near_turn_kernel,
        out_shape=(
            jax.ShapeDtypeStruct((2, ROWS, COLS, CH), F32),
            jax.ShapeDtypeStruct((3 * PART, 4 * ROWS * COLS), BF16),
        ),
        in_specs=[SMEM] + [VMEM] * 7,
        out_specs=(VMEM, VMEM),
        scratch_shapes=[conv_scratch()["spread"]],
        compiler_params=params(),
        cost_estimate=cost(CONV_FLOPS / 4, 6 << 20),
        name="transposed_near",
    )(pos, near, acc, w9, *clips)


def correlate(turned, grads, b):
    width = ROWS * COLS
    rows = ROWS if b == 1 else ROWS - 1
    src = 1 if b == 2 else 0
    dst = 1 if b == 0 else 0
    left = []
    for a in range(3):
        parts = []
        for f in range(2):
            at = (a + f) * width + src * COLS
            parts.append(turned[:, at : at + rows * COLS])
        left.append(jnp.concatenate(parts, axis=1))
    left = jnp.concatenate(left, axis=0)
    right = [g[dst : dst + rows].reshape(rows * COLS, CH) for g in grads]
    return jnp.dot(left, jnp.concatenate(right, axis=0), preferred_element_type=F32)


def backward_kernel(
    pos, i0, i1, i2, i3, inside, turn_c, s0, s1, pre, weight, head, sent, kept,
    spread, acc, turn_i, pgb, total,
):
    core = pos[1]
    grads = (i0, i1, i2, i3)
    part_transposed(grads, pos, turn_i)
    side_taps(core, i3, weight, inside, acc, spread)
    sum_bias = jnp.zeros((8, CH), F32)
    sum_head = jnp.zeros((8, CH), F32)
    for f in range(2):
        for r in range(ROWS):
            back = PENALTY * acc[f, r]
            value = pre[f, r]
            sig = jax.nn.sigmoid(value)
            slope = sig * (1.0 + value * (1.0 - sig))
            curve = sig * (1.0 - sig) * (2.0 + value * (1.0 - 2.0 * sig))
            grad = back * head[...] * curve
            pgb[f, r] = grad.astype(BF16)
            sum_bias = sum_bias + jnp.sum(grad.reshape(COLS // 8, 8, CH), axis=0)
            sum_head = sum_head + jnp.sum((back * slope).reshape(COLS // 8, 8, CH), axis=0)
    total_bias = jnp.sum(sum_bias, axis=0, keepdims=True)
    total_head = jnp.sum(sum_head, axis=0, keepdims=True)
    row = lax.broadcasted_iota(jnp.int32, (8, CH), 0)
    small_bias = jnp.where(row == 0, total_bias, 0.0)
    small_head = jnp.where(row == 0, total_head, 0.0)
    blocks = []
    for b in range(3):
        block = PENALTY * correlate(turn_i, (s0, s1), b) + correlate(turn_c, (pgb.at[0], pgb.at[1]), b)
        blocks.append(block)
    for b, block in enumerate(blocks):
        total[b * 9 * PART : (b + 1) * 9 * PART] = block

    def store(out, h):
        lanes = slice(h * 128, (h + 1) * 128)
        for k in range(27):
            a, b, d = k // 9, (k // 3) % 3, k % 3
            at = ((b * 3 + a) * 3 + d) * PART
            out[k * 8 : (k + 1) * 8] = total[at : at + PART, lanes].reshape(PART // 8, 8, 128)
        out[TILES] = small_bias[:, lanes]
        out[TILES + 1] = small_head[:, lanes]
        out[TILES + 2 :] = jnp.zeros((PIECE * PIECES - TILES - 2, 8, 128), F32)

    @pl.when(core == 0)
    def _():
        store(kept, 0)
        store(sent, 1)

    @pl.when(core == 1)
    def _():
        store(kept, 1)
        store(sent, 0)


def backward(pos, grads, inside, turn_c, score, pre, w9, head):
    s = conv_scratch()
    return pl.pallas_call(
        backward_kernel,
        out_shape=(jax.ShapeDtypeStruct((PIECE * PIECES, 8, 128), F32),) * 2,
        in_specs=[SMEM] + [VMEM] * 11,
        out_specs=(VMEM, VMEM),
        scratch_shapes=[
            s["spread"],
            s["acc"],
            pltpu.VMEM((3 * PART, 4 * ROWS * COLS), BF16),
            pltpu.VMEM((2, ROWS, COLS, CH), BF16),
            pltpu.VMEM((27 * PART, CH), F32),
        ],
        compiler_params=params(),
        cost_estimate=cost(CONV_FLOPS * 1.6, 10 << 20),
        name="backward",
    )(pos, *grads, inside, turn_c, *score, pre, w9, head)


def relative(distance):
    return jnp.where(distance == 0, 0, jnp.where(distance == 3, 1, distance + 1))


def encode(value):
    most = jnp.max(jnp.abs(value), axis=1, keepdims=True)
    wide = (most * 1.004).astype(BF16).astype(F32)
    inverse = jnp.where(wide > 1e-37, 1.0 / jnp.maximum(wide, 1e-37), 0.0)
    code = jnp.exp2(jnp.abs(value) * inverse * SPAN - SPAN / 2)
    code = jnp.where(value < 0, -code, code).reshape(PIECE * 8, 128)
    tail = jnp.concatenate([wide.reshape(PIECE, 128), jnp.zeros((1, 128), F32)], axis=0)
    return jnp.concatenate([code, tail], axis=0).astype(BF16)


def encode_terms_kernel(kept, received, out):
    def step(n, _):
        at = pl.ds(n * PIECE, PIECE)
        out[n] = encode(kept[at] + received[at])
        return 0

    lax.fori_loop(0, PIECES, step, 0, unroll=4)


def encode_terms(kept, received):
    return pl.pallas_call(
        encode_terms_kernel,
        out_shape=jax.ShapeDtypeStruct((PIECES, CODED, 128), BF16),
        in_specs=[VMEM, VMEM],
        out_specs=VMEM,
        compiler_params=params(4 << 20),
        cost_estimate=cost(1e6, 3 << 20),
        name="encode_terms",
    )(kept, received)


def recode_kernel(pieces, out):
    def step(n, total):
        more = decode(pieces[n])
        return tuple(t + m for t, m in zip(total, more))

    zero = tuple(jnp.zeros((8, 128), F32) for _ in range(PIECE))
    total = lax.fori_loop(0, PIECES, step, zero, unroll=4)
    line = encode(jnp.stack(total))
    for n in range(8):
        out[n] = line


def recode(pieces):
    return pl.pallas_call(
        recode_kernel,
        out_shape=jax.ShapeDtypeStruct((8, CODED, 128), BF16),
        in_specs=[VMEM],
        out_specs=VMEM,
        compiler_params=params(4 << 20),
        cost_estimate=cost(1e6, 1 << 19),
        name="recode",
    )(pieces)


def decode(line):
    wide = line.astype(F32)
    level = jnp.log2(jnp.abs(wide[: PIECE * 8])) * (1.0 / SPAN) + 0.5
    level = jnp.where(wide[: PIECE * 8] < 0, -level, level)
    return [
        level[8 * j : 8 * j + 8] * wide[PIECE * 8 + j : PIECE * 8 + j + 1] for j in range(PIECE)
    ]


def assemble_kernel(pos, mine, other, out, small):
    x, core, y = pos[0], pos[1], pos[2]
    part = pl.program_id(0)
    at_x = relative(lax.rem(part - x + 4, 4))
    for ref, held in ((mine, core), (other, 1 - core)):
        lane = pl.ds(pl.multiple_of(held * 128, 128), 128)
        for row in range(4):
            at_y = relative(lax.rem(row - y + 4, 4))
            place = jnp.where(held == 1, at_x * 4 + at_y, at_y * 4 + at_x)
            for z in range(8):
                piece = ((row // 2) * 8 + z) * 2 + row % 2
                for j, value in enumerate(decode(ref[place, z])):
                    tile = piece * PIECE + j
                    if tile < TILES:
                        out[tile // 8, 0, tile % 8, :, lane] = value
                    elif tile < TILES + 2:
                        at = (tile - TILES) * 8
                        small[at : at + 8, lane] = value


def assemble(pos, mine, other):
    return pl.pallas_call(
        assemble_kernel,
        grid=(ROWS,),
        out_shape=(
            jax.ShapeDtypeStruct((27, ROWS, 8, 8, CH), F32),
            jax.ShapeDtypeStruct((16, CH), F32),
        ),
        in_specs=[SMEM, VMEM, VMEM],
        out_specs=(
            pl.BlockSpec((27, 1, 8, 8, CH), lambda i: (0, i, 0, 0, 0)),
            pl.BlockSpec((16, CH), lambda i: (0, 0)),
        ),
        compiler_params=params(),
        cost_estimate=cost(1e6, 15 << 20),
        name="assemble",
    )(pos, mine, other)


def ring_gather(value, plan, direct=False):
    below = permute(value, plan(1))
    above = permute(value, plan(-1))
    if direct:
        return jnp.stack([value, below, above, permute(value, plan(2))])
    half = value.shape[0] // 2
    across_low = permute(below[:half], plan(1))
    across_high = permute(above[half:], plan(-1))
    across = jnp.concatenate([across_low, across_high], axis=0)
    return jnp.stack([value, below, above, across])


def per_device(clips, weight, bias, head):
    x = lax.axis_index("x")
    core = lax.axis_index("c")
    y = lax.axis_index("yh") * 2 + lax.axis_index("yl")
    pos = jnp.stack([x, core, y]).astype(jnp.int32)
    own = clips.reshape(2, COLS, CH)
    below = permute(own, along_x(1))
    above = permute(own, along_x(-1))
    across = permute(own, along_x(2))
    turned, weight, bias, head = turn_weights(weight, bias.reshape(1, CH), head.reshape(1, CH))
    turned = turned.reshape(3, 3, 3 * CH, CH)
    w9 = weight.reshape(3, 3, 3 * CH, CH)

    c1, c2, near, far = gather_rows(pos, own, below, above, across, bias)
    c0, c3 = trade(near, far)
    acc = add_near(pos, c0, inner(c1, c2, w9, "forward_inner"), w9, "forward_near")
    pre, s0, s1, near, far = forward(pos, c3, acc, w9, bias, head)
    near, far = trade(near, far)
    acc = inner(s0, s1, turned, "transposed_inner")
    acc, turn_c = add_near_turn(pos, near, acc, turned, (c0, c1, c2, c3))
    i1, i2, edge, rim = transposed(pos, far, acc, turned)
    i0, i3 = trade(edge, rim)
    inside = inner(i1, i2, w9, "backward_inner")
    inside = add_near(pos, i0, inside, w9, "backward_near")
    sent, kept = backward(pos, (i0, i1, i2, i3), inside, turn_c, (s0, s1), pre, w9, head)
    coded = encode_terms(kept, permute(sent, swap_core))
    pieces = lax.all_to_all(coded, PLANE, 0, 0, tiled=True)
    line = lax.all_to_all(recode(pieces), "z", 0, 0, tiled=True)
    block = ring_gather(line, split_first, direct=True)
    mine = ring_gather(block.reshape(32, CODED, 128), split_second)
    mine = mine.reshape(16, 8, CODED, 128)
    other = permute(mine, swap_core)
    grad_weight, small = assemble(pos, mine, other)
    return grad_weight.reshape(3, 3, 3, CH, CH), small[0], small[8]


def solution(mesh):
    fine = Mesh(mesh.devices.reshape(2, 8, 2, 2, 4), ALL)
    return jax.shard_map(
        per_device,
        mesh=fine,
        in_specs=(P("yh", CHAIN, "x", None, None), P(), P(), P()),
        out_specs=(P(), P(), P()),
        check_vma=False,
    )
```
